16 devices in a mesh: dp: 2 (over y, z), ep: 8 (over x, core).
Axes of the slice: x: 4, y: 2, z: 1, core: 2. Of those that a mesh axis runs over, the one named last changes fastest.
The devices are a block of a 4x4x8 slice.
Arguments:
- tok_in: bfloat16 [2048, 2048], P(('dp', 'ep')), parts along dimension 0
- lat_cache: bfloat16 [2048, 64, 512], P(('dp', 'ep')), parts along dimension 0
- rope_cache: bfloat16 [2048, 64, 64], P(('dp', 'ep')), parts along dimension 0
- tok_pos: int32 [2048], P(('dp', 'ep')), parts along dimension 0
- expert_ids: int32 [2048, 6], P(('dp', 'ep')), parts along dimension 0
- attn_gain: bfloat16 [2048], replicated
- w_query: bfloat16 [2048, 3072], replicated
- w_kvdown: bfloat16 [2048, 576], replicated
- w_ukey: bfloat16 [16, 128, 512], replicated
- w_uval: bfloat16 [16, 512, 128], replicated
- w_out: bfloat16 [2048, 2048], replicated
- ffn_gain: bfloat16 [2048], replicated
- w_router: bfloat16 [2048, 64], replicated
- sh_gate: bfloat16 [2048, 2816], replicated
- sh_up: bfloat16 [2048, 2816], replicated
- sh_down: bfloat16 [2816, 2048], replicated
- ex_gate: bfloat16 [64, 2048, 1408], P('ep')
- ex_up: bfloat16 [64, 2048, 1408], P('ep')
- ex_down: bfloat16 [64, 1408, 2048], P('ep')
Outputs:
- output 1: bfloat16 [2048, 2048], P(('dp', 'ep')), parts along dimension 0
- output 2: bfloat16 [2048, 64, 512], P(('dp', 'ep')), parts along dimension 0
- output 3: bfloat16 [2048, 64, 64], P(('dp', 'ep')), parts along dimension 0
There are 2 independent parts. The reference program is written for one: setup_inputs(seed, part) draws one part's arguments, and reference() takes and returns one part's arrays. A program takes and returns all parts, laid end to end along the dimension named above; an argument that names none is the same for every part.
All inputs are finite; a program needn't handle non-finite values.
Results may differ from the reference program's by a relative error of at most 0.0130158.
Values are sent between devices in bfloat16 or wider.
A program may use at most 768 MiB of HBM per device.

```python
import jax
import jax.numpy as jnp
from jax import lax

D_MODEL = 2048
EXP_FF = 1408
NUM_EXPERTS = 64
TOP_K = 6
SHARED_FF = 2816
NUM_HEADS = 16
NOPE_DIM = 128
ROPE_DIM = 64
V_DIM = 128
KV_RANK = 512
TOKENS_DEV = 128
SEQ_LEN = 64
EP_SIZE = 8

NUM_TOKENS = EP_SIZE * TOKENS_DEV
QK_DIM = NOPE_DIM + ROPE_DIM
ATTN_SCALE = QK_DIM ** -0.5
ROUTE_SCALE = 2.827
ROPE_BASE = 10000.0
NORM_EPS = 1e-6


def unit_norm(values):
    mean_sq = jnp.mean(jnp.square(values), axis=-1, keepdims=True)
    return values * lax.rsqrt(mean_sq + NORM_EPS)


def rms_norm(values, gain_vec):
    return unit_norm(values) * gain_vec.astype(jnp.float32)


def rope_rotate(values, angle_rad):
    half_dim = values.shape[-1] // 2
    x_first = values[..., :half_dim]
    x_second = values[..., half_dim:]
    cos_part = jnp.cos(angle_rad)
    sin_part = jnp.sin(angle_rad)
    return jnp.concatenate([x_first * cos_part - x_second * sin_part, x_second * cos_part + x_first * sin_part], axis=-1)


def draw_routing(key):
    cap_slots = max(2, -(-2 * TOKENS_DEV * TOP_K // NUM_EXPERTS))
    pick_total = TOKENS_DEV * TOP_K
    hot_count = pick_total // (2 * cap_slots)
    rest_picks = pick_total - hot_count * cap_slots
    cold_count = NUM_EXPERTS - hot_count
    rank_ids = jnp.arange(NUM_EXPERTS)
    extra_one = ((rank_ids >= hot_count) & (rank_ids < hot_count + rest_picks % cold_count)).astype(jnp.int32)
    count_per = jnp.where(rank_ids < hot_count, cap_slots, rest_picks // cold_count + extra_one)
    slot_ends = jnp.cumsum(count_per)
    slot_rank = jnp.sum((jnp.arange(pick_total)[:, None] >= slot_ends[None, :]).astype(jnp.int32), axis=1)
    rank_table = slot_rank.reshape(TOP_K, TOKENS_DEV).T
    key_perm, key_rows, key_pos, key_high, key_low = jax.random.split(key, 5)
    expert_perm = jax.random.permutation(key_perm, NUM_EXPERTS)
    row_perms = jax.vmap(lambda sub_key: jax.random.permutation(sub_key, TOKENS_DEV))(jax.random.split(key_rows, EP_SIZE))
    rank_rows = rank_table[row_perms]
    expert_ids = expert_perm[rank_rows].reshape(NUM_TOKENS, TOP_K).astype(jnp.int32)
    pos_draw = jax.random.randint(key_pos, (NUM_TOKENS,), SEQ_LEN // 4, SEQ_LEN)
    high_slot = jax.random.randint(key_high, (), 0, NUM_TOKENS)
    low_slot = (high_slot + jax.random.randint(key_low, (), 1, NUM_TOKENS)) % NUM_TOKENS
    tok_ids = jnp.arange(NUM_TOKENS)
    tok_pos = jnp.where(tok_ids == high_slot, SEQ_LEN - 1, jnp.where(tok_ids == low_slot, SEQ_LEN // 4, pos_draw)).astype(jnp.int32)
    return expert_ids, tok_pos


def setup_inputs(seed: int = 0, part: int = 0) -> dict:
    base_key = jax.random.key(seed)
    part_keys = jax.random.split(jax.random.fold_in(base_key, part), 4)
    weight_keys = jax.random.split(base_key, 16)
    expert_ids, tok_pos = draw_routing(jax.random.fold_in(part_keys[0], 1))

    def gain_draw(key, size, center):
        return (center + 0.2 * jax.random.normal(key, (size,), jnp.float32)).astype(jnp.bfloat16)

    def weight_draw(key, shape, fan_in, factor):
        return (jax.random.normal(key, shape, jnp.float32) * factor * fan_in ** -0.5).astype(jnp.bfloat16)

    tok_in = jax.random.normal(part_keys[1], (NUM_TOKENS, D_MODEL), jnp.float32).astype(jnp.bfloat16)
    lat_cache = (1.3 * jax.random.normal(part_keys[2], (NUM_TOKENS, SEQ_LEN, KV_RANK), jnp.float32)).astype(jnp.bfloat16)
    rope_cache = jax.random.normal(part_keys[3], (NUM_TOKENS, SEQ_LEN, ROPE_DIM), jnp.float32).astype(jnp.bfloat16)
    return {
        'tok_in': tok_in,
        'lat_cache': lat_cache,
        'rope_cache': rope_cache,
        'tok_pos': tok_pos,
        'expert_ids': expert_ids,
        'attn_gain': gain_draw(weight_keys[0], D_MODEL, 1.0),
        'w_query': weight_draw(weight_keys[1], (D_MODEL, NUM_HEADS * QK_DIM), D_MODEL, 1.0),
        'w_kvdown': weight_draw(weight_keys[2], (D_MODEL, KV_RANK + ROPE_DIM), D_MODEL, 1.0),
        'w_ukey': weight_draw(weight_keys[4], (NUM_HEADS, NOPE_DIM, KV_RANK), NOPE_DIM, 1.0),
        'w_uval': weight_draw(weight_keys[5], (NUM_HEADS, KV_RANK, V_DIM), KV_RANK, 1.0),
        'w_out': weight_draw(weight_keys[6], (NUM_HEADS * V_DIM, D_MODEL), NUM_HEADS * V_DIM, 1.0),
        'ffn_gain': gain_draw(weight_keys[7], D_MODEL, 1.0),
        'w_router': weight_draw(weight_keys[8], (D_MODEL, NUM_EXPERTS), D_MODEL, 2.0),
        'sh_gate': weight_draw(weight_keys[9], (D_MODEL, SHARED_FF), D_MODEL, 1.0),
        'sh_up': weight_draw(weight_keys[10], (D_MODEL, SHARED_FF), D_MODEL, 1.0),
        'sh_down': weight_draw(weight_keys[11], (SHARED_FF, D_MODEL), SHARED_FF, 1.0),
        'ex_gate': weight_draw(weight_keys[12], (NUM_EXPERTS, D_MODEL, EXP_FF), D_MODEL, 1.0),
        'ex_up': weight_draw(weight_keys[13], (NUM_EXPERTS, D_MODEL, EXP_FF), D_MODEL, 1.0),
        'ex_down': weight_draw(weight_keys[14], (NUM_EXPERTS, EXP_FF, D_MODEL), EXP_FF, 1.0),
    }


def reference(tok_in, lat_cache, rope_cache, tok_pos, expert_ids, attn_gain, w_query, w_kvdown, w_ukey, w_uval, w_out, ffn_gain, w_router, sh_gate, sh_up, sh_down, ex_gate, ex_up, ex_down):
    x_wide = tok_in.astype(jnp.float32)
    x_norm = rms_norm(x_wide, attn_gain).astype(jnp.bfloat16)
    q_all = jnp.dot(x_norm, w_query, preferred_element_type=jnp.float32).astype(jnp.bfloat16).reshape(NUM_TOKENS, NUM_HEADS, QK_DIM)
    kv_all = jnp.dot(x_norm, w_kvdown, preferred_element_type=jnp.float32)
    inv_freq = ROPE_BASE ** (-(2.0 * jnp.arange(ROPE_DIM // 2)) / ROPE_DIM)
    angle_rad = tok_pos.astype(jnp.float32)[:, None] * inv_freq[None, :]
    lat_new = unit_norm(kv_all[:, :KV_RANK]).astype(jnp.bfloat16)
    rope_new = rope_rotate(kv_all[:, KV_RANK:], angle_rad).astype(jnp.bfloat16)
    q_rope = rope_rotate(q_all[:, :, NOPE_DIM:].astype(jnp.float32), angle_rad[:, None, :]).astype(jnp.bfloat16)
    q_lat = jnp.einsum('bhn,hnc->bhc', q_all[:, :, :NOPE_DIM].astype(jnp.float32), w_ukey.astype(jnp.float32)).astype(jnp.bfloat16)
    seq_ids = jnp.arange(SEQ_LEN)
    at_pos = (seq_ids[None, :] == tok_pos[:, None])[:, :, None]
    lat_out = jnp.where(at_pos, lat_new[:, None, :], lat_cache)
    rope_out = jnp.where(at_pos, rope_new[:, None, :], rope_cache)

    def one_token(item_tuple):
        q_lat_t, q_rope_t, lat_t, rope_t, pos_t = item_tuple
        scores = jnp.dot(q_lat_t, lat_t.T, preferred_element_type=jnp.float32)
        scores = scores + jnp.dot(q_rope_t, rope_t.T, preferred_element_type=jnp.float32)
        scores = scores * ATTN_SCALE
        visible = seq_ids[None, :] <= pos_t
        scores = jnp.where(visible, scores, -jnp.inf)
        prob_mat = jax.nn.softmax(scores, axis=-1).astype(jnp.bfloat16)
        return jnp.dot(prob_mat, lat_t, preferred_element_type=jnp.float32).astype(jnp.bfloat16)

    o_lat = lax.map(one_token, (q_lat, q_rope, lat_out, rope_out, tok_pos))
    o_heads = jnp.einsum('bhc,hcv->bhv', o_lat.astype(jnp.float32), w_uval.astype(jnp.float32)).astype(jnp.bfloat16)
    attn_out = jnp.dot(o_heads.reshape(NUM_TOKENS, NUM_HEADS * V_DIM), w_out, preferred_element_type=jnp.float32)
    resid_bf = (x_wide + attn_out).astype(jnp.bfloat16)
    h_norm = rms_norm(resid_bf.astype(jnp.float32), ffn_gain).astype(jnp.bfloat16)
    gate_prob = jax.nn.sigmoid(jnp.dot(h_norm, w_router, preferred_element_type=jnp.float32))
    chosen = jnp.take_along_axis(gate_prob, expert_ids, axis=1)
    route_w = ROUTE_SCALE * chosen / jnp.sum(chosen, axis=1, keepdims=True)
    sh_act = (jax.nn.silu(jnp.dot(h_norm, sh_gate, preferred_element_type=jnp.float32)) * jnp.dot(h_norm, sh_up, preferred_element_type=jnp.float32)).astype(jnp.bfloat16)
    shared_out = jnp.dot(sh_act, sh_down, preferred_element_type=jnp.float32)
    flat_rows = jnp.repeat(h_norm, TOP_K, axis=0)
    flat_ids = expert_ids.reshape(NUM_TOKENS * TOP_K)

    def one_choice(item_tuple):
        row_vec, expert = item_tuple
        row_mat = row_vec[None, :]
        gate_val = jnp.dot(row_mat, ex_gate[expert], preferred_element_type=jnp.float32)
        up_val = jnp.dot(row_mat, ex_up[expert], preferred_element_type=jnp.float32)
        act_val = (jax.nn.silu(gate_val) * up_val).astype(jnp.bfloat16)
        return jnp.dot(act_val, ex_down[expert], preferred_element_type=jnp.float32).astype(jnp.bfloat16)[0]

    choice_out = lax.map(one_choice, (flat_rows, flat_ids)).reshape(NUM_TOKENS, TOP_K, D_MODEL)
    routed = jnp.sum(route_w[:, :, None] * choice_out.astype(jnp.float32), axis=1)
    out_hidden = (resid_bf.astype(jnp.float32) + shared_out + routed).astype(jnp.bfloat16)
    return (out_hidden, lat_out, rope_out)
```

```python
import functools

import jax
import jax.numpy as jnp
from jax import lax
from jax.experimental import pallas as pl
from jax.experimental.pallas import tpu as pltpu
from jax.sharding import PartitionSpec as P

ROUTE_SCALE = 2.827
ROPE_BASE = 10000.0
NORM_EPS = 1e-6
F32 = jnp.float32
BF16 = jnp.bfloat16
VMEM_LIMIT = 67_043_328

GROUP = 8
CHUNK = 256


def unit_norm(values):
    mean_sq = jnp.mean(jnp.square(values), axis=-1, keepdims=True)
    return values * lax.rsqrt(mean_sq + NORM_EPS)


def mm(a, b):
    return jnp.dot(a, b, preferred_element_type=F32)


def mm_nt(a, b):
    return lax.dot_general(a, b, (((1,), (1,)), ((), ())), preferred_element_type=F32)


def attention_kernel(
    pos_smem, x_ref, pos_ref, freq_ref, gain_a_ref, gain_f_ref, lat_ref, rope_ref,
    wq_hbm, wkv_hbm, wuk_hbm, wuv_hbm, wo_hbm,
    lat_out, rope_out, resid_ref, h_ref,
    wq, wkv, wuk_even, wuk_odd, wuv, wo, qc, qr, olat, c_scr, k_scr, heads_scr, sem,
):
    step = pl.program_id(0)
    heads, nope, rank = wuk_hbm.shape
    rope_dim = rope_ref.shape[-1]
    rows, d_model = x_ref.shape
    seq = lat_ref.shape[1]
    pairs = heads // 2
    pair_cols = 2 * (nope + rope_dim)
    per_copy = 2
    copies = pairs // per_copy
    wide = per_copy * pair_cols

    def q_copy(i):
        cols = pl.ds(i * wide, wide)
        return pltpu.make_async_copy(wq_hbm.at[:, cols], wq.at[:, cols], sem.at[i])

    kv_copy = pltpu.make_async_copy(wkv_hbm, wkv, sem.at[copies])
    uv_copy = pltpu.make_async_copy(wuv_hbm, wuv, sem.at[copies + 1])
    wo_copy = pltpu.make_async_copy(wo_hbm, wo, sem.at[copies + 2])

    def uk_copies(i):
        even = pltpu.make_async_copy(wuk_hbm.at[2 * i], wuk_even.at[i], sem.at[copies + 3 + 2 * i])
        odd = pltpu.make_async_copy(wuk_hbm.at[2 * i + 1], wuk_odd.at[i, rope_dim : rope_dim + nope], sem.at[copies + 4 + 2 * i])
        return even, odd

    @pl.when(step == 0)
    def _():
        kv_copy.start()
        for i in range(copies):
            q_copy(i).start()
            for j in range(per_copy):
                for c in uk_copies(i * per_copy + j):
                    c.start()
        uv_copy.start()
        wo_copy.start()
        zero = jnp.zeros((pairs, rope_dim, rank), BF16)
        wuk_odd[:, :rope_dim] = zero
        wuk_odd[:, rope_dim + nope :] = zero
        x_norm = (unit_norm(x_ref[...].astype(F32)) * gain_a_ref[...].astype(F32)).astype(BF16)
        angle = pos_ref[...].astype(F32) * freq_ref[...]
        cos, sin = jnp.cos(angle), jnp.sin(angle)
        lane = lax.broadcasted_iota(jnp.int32, (rows, 2 * rope_dim), 1)
        first = lax.rem(lane, rope_dim) < rope_dim // 2

        def rope(v):
            ahead = pltpu.roll(v, 2 * rope_dim - rope_dim // 2, 1)
            behind = pltpu.roll(v, rope_dim // 2, 1)
            return (v * cos + jnp.where(first, -ahead, behind) * sin).astype(BF16)

        kv_copy.wait()
        kv = mm(x_norm, wkv[...])
        c_scr[...] = unit_norm(kv[:, :rank]).astype(BF16).astype(F32)
        k_part = kv[:, rank:]
        k_scr[...] = rope(jnp.concatenate([k_part, k_part], axis=1)).astype(F32)
        for i in range(pairs):
            if i % per_copy == 0:
                q_copy(i // per_copy).wait()
            for c in uk_copies(i):
                c.wait()
            q = mm(x_norm, wq[:, i * pair_cols : (i + 1) * pair_cols]).astype(BF16)
            qc[2 * i] = mm(q[:, :nope], wuk_even[i]).astype(BF16).astype(F32)
            qc[2 * i + 1] = mm(q[:, nope:], wuk_odd[i]).astype(BF16).astype(F32)
            both = jnp.where(lane < rope_dim, q[:, nope : 2 * nope].astype(F32), q[:, 2 * nope :].astype(F32))
            turned = rope(both).astype(F32)
            qr[2 * i] = turned
            qr[2 * i + 1] = pltpu.roll(turned, rope_dim, 1)

    at = pl.ds(pl.multiple_of(step * GROUP, GROUP), GROUP)
    c_new = c_scr[at, :]
    k_new = k_scr[at, :rope_dim]
    slot_lat = lax.broadcasted_iota(jnp.int32, (seq, rank), 0)
    slot_rope = lax.broadcasted_iota(jnp.int32, (seq, rope_dim), 0)
    for t in range(GROUP):
        pos = pos_smem[step * GROUP + t]
        lat_out[t] = jnp.where(slot_lat == pos, c_new[t : t + 1, :], lat_ref[t].astype(F32)).astype(BF16)
        rope_out[t] = jnp.where(slot_rope == pos, k_new[t : t + 1, :], rope_ref[t].astype(F32)).astype(BF16)
    keys = lat_out[...].reshape(GROUP * seq, rank)
    keys_rope = rope_out[...].reshape(GROUP * seq, rope_dim)
    q_lat = qc[:, at, :].reshape(heads * GROUP, rank).astype(BF16)
    q_rope = qr[:, at, :].reshape(heads * GROUP, 2 * rope_dim).astype(BF16)[:, :rope_dim]
    scores = (mm_nt(q_lat, keys) + mm_nt(q_rope, keys_rope)) * (nope + rope_dim) ** -0.5
    key_id = lax.broadcasted_iota(jnp.int32, (GROUP, GROUP * seq), 1)
    low = lax.broadcasted_iota(jnp.int32, (GROUP, GROUP * seq), 0) * seq
    seen = (key_id >= low) & (key_id <= low + pos_ref[at, :])
    scores = jnp.where(seen[None], scores.reshape(heads, GROUP, GROUP * seq), -jnp.inf)
    expd = jnp.exp(scores - jnp.max(scores, axis=-1, keepdims=True))
    prob = (expd / jnp.sum(expd, axis=-1, keepdims=True)).astype(BF16)
    out = mm(prob.reshape(heads * GROUP, GROUP * seq), keys).astype(BF16).astype(F32)
    olat[:, at, :] = out.reshape(heads, GROUP, rank)

    @pl.when(step == pl.num_programs(0) - 1)
    def _():
        uv_copy.wait()
        v_dim = wuv.shape[-1]
        for h in range(heads):
            heads_scr[:, h * v_dim : (h + 1) * v_dim] = mm(olat[h].astype(BF16), wuv[h]).astype(BF16)
        wo_copy.wait()
        piece = 512
        for n in range(0, d_model, piece):
            part = mm(heads_scr[...], wo[:, n : n + piece])
            resid_ref[:, n : n + piece] = (x_ref[:, n : n + piece].astype(F32) + part).astype(BF16)
        h_ref[...] = (unit_norm(resid_ref[...].astype(F32)) * gain_f_ref[...].astype(F32)).astype(BF16)


def attention(tok_in, lat_cache, rope_cache, tok_pos, attn_gain, w_query, w_kvdown, w_ukey, w_uval, w_out, ffn_gain):
    rows, d_model = tok_in.shape
    _, seq, rank = lat_cache.shape
    rope_dim = rope_cache.shape[-1]
    heads, nope, _ = w_ukey.shape
    v_dim = w_uval.shape[-1]
    inv_freq = ROPE_BASE ** (-(2.0 * jnp.arange(rope_dim // 2)) / rope_dim)
    freq = jnp.tile(inv_freq, 4)[None, :]

    def const(shape):
        return pl.BlockSpec(shape, lambda g, *_: (0,) * len(shape))

    any_spec = pl.BlockSpec(memory_space=pl.ANY)
    lat_spec = pl.BlockSpec((GROUP, seq, rank), lambda g, *_: (g, 0, 0))
    rope_spec = pl.BlockSpec((GROUP, seq, rope_dim), lambda g, *_: (g, 0, 0))
    grid_spec = pltpu.PrefetchScalarGridSpec(
        num_scalar_prefetch=1,
        grid=(rows // GROUP,),
        in_specs=[const((rows, d_model)), const((rows, 1)), const((1, 2 * rope_dim)), const((1, d_model)), const((1, d_model)),
                  lat_spec, rope_spec] + [any_spec] * 5,
        out_specs=[lat_spec, rope_spec, const((rows, d_model)), const((rows, d_model))],
        scratch_shapes=[
            pltpu.VMEM(w_query.shape, BF16),
            pltpu.VMEM(w_kvdown.shape, BF16),
            pltpu.VMEM((heads // 2, nope, rank), BF16),
            pltpu.VMEM((heads // 2, nope + 2 * rope_dim, rank), BF16),
            pltpu.VMEM(w_uval.shape, BF16),
            pltpu.VMEM(w_out.shape, BF16),
            pltpu.VMEM((heads, rows, rank), F32),
            pltpu.VMEM((heads, rows, 2 * rope_dim), F32),
            pltpu.VMEM((heads, rows, rank), F32),
            pltpu.VMEM((rows, rank), F32),
            pltpu.VMEM((rows, 2 * rope_dim), F32),
            pltpu.VMEM((rows, heads * v_dim), BF16),
            pltpu.SemaphoreType.DMA((heads // 4 + 3 + heads,)),
        ],
    )
    return pl.pallas_call(
        attention_kernel,
        name="attention",
        grid_spec=grid_spec,
        out_shape=[
            jax.ShapeDtypeStruct(lat_cache.shape, BF16),
            jax.ShapeDtypeStruct(rope_cache.shape, BF16),
            jax.ShapeDtypeStruct((rows, d_model), BF16),
            jax.ShapeDtypeStruct((rows, d_model), BF16),
        ],
        compiler_params=pltpu.CompilerParams(vmem_limit_bytes=VMEM_LIMIT, dimension_semantics=("arbitrary",)),
    )(tok_pos, tok_in, tok_pos[:, None], freq, attn_gain[None, :], ffn_gain[None, :], lat_cache, rope_cache,
      w_query, w_kvdown, w_ukey, w_uval, w_out)


def moe_kernel(
    ep, slots, h_in, resid_ref, ids_ref, wr_ref,
    shg, shu, shd, exg, exu, exd,
    out_ref,
    wbuf, h_all, w_send, w_all, pick, weigh, comb, x_all, acts, acts_sh, e_buf,
    part, part_peer, from_peer, transit, final, sh_acc,
    w_sem, b_sem, ag_send, ag_recv, rt_send, rt_recv, rs_send, rs_recv,
):
    rows, d_model = h_in.shape
    local, _, ff = exg.shape
    chips = ep // 2
    half = rows // 2
    pair_slots = 2 * slots
    shared_parts = shg.shape[1] // ff
    chunks = d_model // CHUNK
    per_slot = ff // CHUNK
    me = lax.axis_index("ep")
    chip, core = me // 2, lax.rem(me, 2)

    def device(chip_step, other_core):
        side = 1 - core if other_core else core
        return lax.rem(chip + chip_step, chips) * 2 + side

    right, left, peer = device(1, False), device(chips - 1, False), device(0, True)

    def remote(src, dst, send, recv, to):
        return pltpu.make_async_remote_copy(
            src_ref=src, dst_ref=dst, send_sem=send, recv_sem=recv,
            device_id={"ep": to}, device_id_type=pl.DeviceIdType.MESH)

    def shared_copies(i):
        cols = pl.ds(i * ff, ff)
        return [pltpu.make_async_copy(src.at[:, cols], wbuf.at[i % 2, k], w_sem.at[i % 2, k]) for k, src in enumerate((shg, shu))]

    def expert_copies(e):
        s = lax.rem(e, 2)
        return [pltpu.make_async_copy(src.at[e], wbuf.at[s, k], w_sem.at[s, k]) for k, src in enumerate((exg, exu))]

    def down_copy(c, k):
        s = lax.rem(c, 2)
        cols = pl.ds(pl.multiple_of(c * CHUNK, CHUNK), CHUNK)
        src = exd.at[k, :, cols] if k < local else shd.at[pl.ds((k - local) * ff, ff), cols]
        return pltpu.make_async_copy(src, down_tile(c, k), b_sem.at[s, k])

    def down_tile(c, k):
        return wbuf.at[lax.rem(c, 2), k // per_slot, pl.ds(0, ff), pl.ds((k % per_slot) * CHUNK, CHUNK)]

    def start_down(c):
        for k in range(local + shared_parts):
            down_copy(c, k).start()

    for i in range(shared_parts):
        for c in shared_copies(i):
            c.start()

    barrier = pltpu.get_barrier_semaphore()
    others = [(dc, oc) for dc in range(chips) for oc in (False, True) if dc or oc]
    for dc, oc in others:
        pl.semaphore_signal(barrier, inc=1, device_id={"ep": device(dc, oc)}, device_id_type=pl.DeviceIdType.MESH)
    pl.semaphore_wait(barrier, len(others))

    top, low = pl.ds(0, half), pl.ds(half, half)
    top_o, low_o = pl.ds(rows, half), pl.ds(rows + half, half)
    back, far = chips - 1, chips - 2

    def gather_copy(i):
        src, dst, to = (
            (h_in, h_all.at[0, pl.ds(rows, rows)], peer),
            (h_in.at[top], h_all.at[back, top], right),
            (h_in.at[low], h_all.at[back, low], right),
            (h_in.at[low], h_all.at[1, low], left),
            (h_in.at[top], h_all.at[1, top], left),
            (h_all.at[back, top], h_all.at[far, top], right),
            (h_all.at[1, low], h_all.at[far, low], left),
            (h_all.at[back, top], h_all.at[back, top_o], peer),
            (h_all.at[1, low], h_all.at[1, low_o], peer),
            (h_all.at[back, low], h_all.at[back, low_o], peer),
            (h_all.at[1, top], h_all.at[1, top_o], peer),
            (h_all.at[far, top], h_all.at[far, top_o], peer),
            (h_all.at[far, low], h_all.at[far, low_o], peer),
        )[i]
        return remote(src, dst, ag_send.at[i], ag_recv.at[i], to)

    for i in range(5):
        gather_copy(i).start()

    logits = mm_nt(wr_ref[...], h_in[...])
    gate = jax.nn.sigmoid(logits)
    expert_id = lax.broadcasted_iota(jnp.int32, logits.shape, 0)
    listed = expert_id == ids_ref[0:1, :]
    for k in range(1, ids_ref.shape[0]):
        listed = listed | (expert_id == ids_ref[k : k + 1, :])
    total = jnp.sum(jnp.where(listed, gate, 0.0), axis=0, keepdims=True)
    w_send[...] = jnp.where(listed, ROUTE_SCALE * gate / total, -1.0)

    def mine(d):
        return pl.ds(pl.multiple_of(d * local, local), local)

    def route_copy(i):
        dc, oc = others[i]
        d = device(dc, oc)
        return remote(w_send.at[mine(d)], w_all.at[(chips - dc) % chips, int(oc)], rt_send.at[i], rt_recv.at[i], d)

    for i in range(len(others)):
        route_copy(i).start()
    w_all[0, 0] = w_send[mine(me), :]
    h_all[0, :rows] = h_in[...]

    def up(x, s, act):
        for n in range(0, ff, 512):
            cols = pl.ds(n, min(512, ff - n))
            g = mm(x[...], wbuf[s, 0, :, cols])
            u = mm(x[...], wbuf[s, 1, :, cols])
            act[:, cols] = (jax.nn.silu(g) * u).astype(BF16)

    earlier = lax.broadcasted_iota(jnp.int32, (rows, rows), 0) < lax.broadcasted_iota(jnp.int32, (rows, rows), 1)
    tri = jnp.where(earlier, 1.0, 0.0).astype(BF16)
    slot_id = lax.broadcasted_iota(jnp.int32, (pair_slots, 2 * rows), 0).astype(F32)

    def place(r):
        ranks, weights = [], []
        for q in range(2):
            w = w_all[r, q]
            has = w >= 0.0
            rank = mm(jnp.where(has, 1.0, 0.0).astype(BF16), tri)
            ranks.append(jnp.where(has, rank + q * slots, -1.0))
            weights.append(w)
        rank, w = jnp.concatenate(ranks, axis=1), jnp.concatenate(weights, axis=1)
        for e in range(local):
            at = pl.ds(e * pair_slots, pair_slots)
            hit = slot_id == rank[e : e + 1, :]
            pick[at, :] = jnp.where(hit, 1.0, 0.0).astype(BF16)
            weigh[at, :] = jnp.where(hit, w[e : e + 1, :], 0.0)
        rest = weigh[...].T
        for k in range(3):
            piece = rest.astype(BF16)
            comb[r, pl.ds(k * 2 * rows, 2 * rows), :] = piece
            rest = rest - piece.astype(F32)

        @pl.loop(0, d_model // 512)
        def _(n):
            cols = pl.ds(pl.multiple_of(n * 512, 512), 512)
            x = mm(pick[...], h_all[r, :, cols]).astype(BF16)
            for e in range(local):
                x_all[e, pl.ds(r * pair_slots, pair_slots), cols] = x[e * pair_slots : (e + 1) * pair_slots]

    def wait_recv(*ids):
        for i in ids:
            gather_copy(i).wait_recv()

    for c in shared_copies(0):
        c.wait()
    up(h_in, 0, acts_sh.at[0])
    for c in expert_copies(0):
        c.start()
    wait_recv(1, 3)
    for i in (5, 6, 7, 8):
        gather_copy(i).start()
    for c in shared_copies(1):
        c.wait()
    up(h_in, 1, acts_sh.at[1])
    for c in expert_copies(1):
        c.start()
    for i in range(len(others)):
        route_copy(i).wait_recv()
    wait_recv(0)
    place(0)
    wait_recv(2, 4)
    for i in (9, 10):
        gather_copy(i).start()
    wait_recv(7, 9)
    place(back)
    wait_recv(8, 10)
    place(1)
    wait_recv(5, 6)
    for i in (11, 12):
        gather_copy(i).start()
    wait_recv(11, 12)
    place(far)

    @pl.loop(0, local)
    def _(e):
        for c in expert_copies(e):
            c.wait()
        up(x_all.at[e], lax.rem(e, 2), acts.at[e])

        @pl.when(e < local - 2)
        def _():
            for c in expert_copies(e + 2):
                c.start()

        @pl.when(e >= local - 2)
        def _():
            start_down(e - (local - 2))

    def rs_copy(i, c):
        src, dst, to = (
            (part_peer.at[c], from_peer.at[c], peer),
            (part.at[c, far, top], transit.at[0, c], right),
            (part.at[c, far, low], transit.at[1, c], left),
            (part.at[c, 1, low], final.at[0, c, low], right),
            (part.at[c, back, top], final.at[1, c, top], left),
            (part.at[c, 1, top], final.at[0, c, top], right),
            (part.at[c, back, low], final.at[1, c, low], left),
        )[i]
        return remote(src, dst, rs_send.at[i, c], rs_recv.at[i, c], to)

    def add_peer(c):
        rs_copy(0, c).wait_recv()
        for r in (far, 1, back):
            part[c, r] += from_peer[c, r]
            if r == far:
                rs_copy(1, c).start()
                rs_copy(2, c).start()
        rs_copy(3, c).start()
        rs_copy(4, c).start()
        part[c, 0] += from_peer[c, 0]

    def pass_on(c):
        rs_copy(1, c).wait_recv()
        part[c, 1, top] += transit[0, c]
        rs_copy(5, c).start()
        rs_copy(2, c).wait_recv()
        part[c, back, low] += transit[1, c]
        rs_copy(6, c).start()

    @pl.loop(0, chunks)
    def _(c):
        for k in range(local):
            down_copy(c, k).wait()
            y = mm(acts[k], down_tile(c, k)[...]).astype(BF16)
            for r in range(chips):
                e_buf[r, k * pair_slots : (k + 1) * pair_slots, :] = y[r * pair_slots : (r + 1) * pair_slots]

        @pl.when(c >= 1)
        def _():
            add_peer(c - 1)

        for r in range(chips):
            z = mm(comb[r], e_buf[r])
            z = z[: 2 * rows] + z[2 * rows : 4 * rows] + z[4 * rows :]
            part[c, r] = z[:rows]
            part_peer[c, r] = z[rows:]
        rs_copy(0, c).start()

        shared = None
        for k in range(local, local + shared_parts):
            down_copy(c, k).wait()
            y = mm(acts_sh[k - local], down_tile(c, k)[...])
            shared = y if shared is None else shared + y
        sh_acc[c] = shared

        @pl.when(c + 2 < chunks)
        def _():
            start_down(c + 2)

        @pl.when(c >= 2)
        def _():
            pass_on(c - 2)

    add_peer(chunks - 1)
    pass_on(chunks - 2)
    pass_on(chunks - 1)
    for c in range(chunks):
        for i in (3, 4, 5, 6):
            rs_copy(i, c).wait_recv()
        cols = pl.ds(c * CHUNK, CHUNK)
        routed = part[c, 0] + final[0, c] + final[1, c]
        out_ref[:, cols] = (resid_ref[:, cols].astype(F32) + sh_acc[c] + routed).astype(BF16)
    for i in range(13):
        gather_copy(i).wait_send()
    for i in range(len(others)):
        route_copy(i).wait_send()

    @pl.loop(0, chunks)
    def _(c):
        for i in range(7):
            rs_copy(i, c).wait_send()


def moe(ep, h_norm, resid, expert_ids, w_router, sh_gate, sh_up, sh_down, ex_gate, ex_up, ex_down):
    rows, d_model = h_norm.shape
    top_k = expert_ids.shape[1]
    num_experts = w_router.shape[1]
    local, _, ff = ex_gate.shape
    chips = ep // 2
    slots = max(2, -(-2 * rows * top_k // num_experts))
    shared_parts = sh_gate.shape[1] // ff
    chunks = d_model // CHUNK
    pair_slots = 2 * slots
    dma = pltpu.SemaphoreType.DMA
    vmem = pl.BlockSpec(memory_space=pltpu.VMEM)
    any_spec = pl.BlockSpec(memory_space=pl.ANY)
    return pl.pallas_call(
        functools.partial(moe_kernel, ep, slots),
        name="experts",
        in_specs=[vmem] * 4 + [any_spec] * 6,
        out_specs=vmem,
        out_shape=jax.ShapeDtypeStruct((rows, d_model), BF16),
        scratch_shapes=[
            pltpu.VMEM((2, 2, d_model, ff), BF16),
            pltpu.VMEM((chips, 2 * rows, d_model), BF16),
            pltpu.VMEM((num_experts, rows), F32),
            pltpu.VMEM((chips, 2, local, rows), F32),
            pltpu.VMEM((local * pair_slots, 2 * rows), BF16),
            pltpu.VMEM((local * pair_slots, 2 * rows), F32),
            pltpu.VMEM((chips, 6 * rows, local * pair_slots), BF16),
            pltpu.VMEM((local, chips * pair_slots, d_model), BF16),
            pltpu.VMEM((local, chips * pair_slots, ff), BF16),
            pltpu.VMEM((shared_parts, rows, ff), BF16),
            pltpu.VMEM((chips, local * pair_slots, CHUNK), BF16),
            pltpu.VMEM((chunks, chips, rows, CHUNK), F32),
            pltpu.VMEM((chunks, chips, rows, CHUNK), F32),
            pltpu.VMEM((chunks, chips, rows, CHUNK), F32),
            pltpu.VMEM((2, chunks, rows // 2, CHUNK), F32),
            pltpu.VMEM((2, chunks, rows, CHUNK), F32),
            pltpu.VMEM((chunks, rows, CHUNK), F32),
            dma((2, 2)), dma((2, local + shared_parts)),
            dma((13,)), dma((13,)), dma((ep - 1,)), dma((ep - 1,)), dma((7, chunks)), dma((7, chunks)),
        ],
        compiler_params=pltpu.CompilerParams(vmem_limit_bytes=VMEM_LIMIT, collective_id=0, has_side_effects=True),
    )(h_norm, resid, expert_ids.T, w_router.T, sh_gate, sh_up, sh_down, ex_gate, ex_up, ex_down)


def solution(mesh):
    ep = mesh.shape["ep"]
    row_one = P(("dp", "ep"))
    row_two = P(("dp", "ep"), None)
    row_three = P(("dp", "ep"), None, None)
    rep_one = P(None)
    rep_two = P(None, None)
    rep_three = P(None, None, None)
    exp_spec = P("ep", None, None)

    def local_step(tok_in, lat_cache, rope_cache, tok_pos, expert_ids, attn_gain, w_query, w_kvdown, w_ukey, w_uval, w_out, ffn_gain, w_router, sh_gate, sh_up, sh_down, ex_gate, ex_up, ex_down):
        lat_out, rope_out, resid, h_norm = attention(tok_in, lat_cache, rope_cache, tok_pos, attn_gain, w_query, w_kvdown, w_ukey, w_uval, w_out, ffn_gain)
        out_hidden = moe(ep, h_norm, resid, expert_ids, w_router, sh_gate, sh_up, sh_down, ex_gate, ex_up, ex_down)
        return out_hidden, lat_out, rope_out

    in_specs = (row_two, row_three, row_three, row_one, row_two, rep_one, rep_two, rep_two, rep_three, rep_three, rep_two, rep_one, rep_two, rep_two, rep_two, rep_two, exp_spec, exp_spec, exp_spec)
    out_specs = (row_two, row_three, row_three)
    return jax.shard_map(local_step, mesh=mesh, in_specs=in_specs, out_specs=out_specs, check_vma=False)
```

```python
import functools
import math

import jax
import jax.numpy as jnp
from jax import lax
from jax.experimental import pallas as pl
from jax.experimental.pallas import tpu as pltpu
from jax.sharding import PartitionSpec as P

ROUTE_SCALE = 2.827
ROPE_BASE = 10000.0
NORM_EPS = 1e-6
F32 = jnp.float32
BF16 = jnp.bfloat16
VMEM_LIMIT = 67_043_328

GROUP = 8
GROUPS = 4
CHUNK = 256
BY_SLOT = 512


def unit_norm(values):
    mean_sq = jnp.mean(jnp.square(values), axis=-1, keepdims=True)
    return values * lax.rsqrt(mean_sq + NORM_EPS)


def mm(a, b):
    return jnp.dot(a, b, preferred_element_type=F32)


def mm_nt(a, b):
    return lax.dot_general(a, b, (((1,), (1,)), ((), ())), preferred_element_type=F32)


def attention_kernel(
    pos_smem, x_ref, pos_ref, gain_a_ref, gain_f_ref, lat_ref,
    rope_hbm, wq_hbm, wkv_hbm, wuk_hbm, wuv_hbm, wo_hbm,
    lat_out, rope_out, resid_ref, h_ref,
    wq, wkv, wuk_even, wuk_odd, wuv, wo, rope_in, rope_keys, qc, q_first, q_second, olat, c_scr, pos_scr, heads_scr, s_scr, p_scr, sem,
):
    step = pl.program_id(0)
    heads, nope, rank = wuk_hbm.shape
    seq, rope_dim, rows = rope_in.shape
    d_model = x_ref.shape[1]
    pairs = heads // 2
    pair_cols = 2 * (nope + rope_dim)
    per_copy = 2
    copies = pairs // per_copy
    wide = per_copy * pair_cols

    def q_copy(i):
        cols = pl.ds(i * wide, wide)
        return pltpu.make_async_copy(wq_hbm.at[:, cols], wq.at[:, cols], sem.at[i])

    kv_copy = pltpu.make_async_copy(wkv_hbm, wkv, sem.at[copies])
    uv_copy = pltpu.make_async_copy(wuv_hbm, wuv, sem.at[copies + 1])
    wo_copy = pltpu.make_async_copy(wo_hbm, wo, sem.at[copies + 2])
    rope_copy = pltpu.make_async_copy(rope_hbm, rope_in, sem.at[copies + 3])

    def uk_copies(i):
        even = pltpu.make_async_copy(wuk_hbm.at[2 * i], wuk_even.at[i], sem.at[copies + 4 + 2 * i])
        odd = pltpu.make_async_copy(wuk_hbm.at[2 * i + 1], wuk_odd.at[i, rope_dim : rope_dim + nope], sem.at[copies + 5 + 2 * i])
        return even, odd

    @pl.when(step == 0)
    def _():
        kv_copy.start()
        rope_copy.start()
        for i in range(copies):
            q_copy(i).start()
            for j in range(per_copy):
                for c in uk_copies(i * per_copy + j):
                    c.start()
        uv_copy.start()
        wo_copy.start()
        zero = jnp.zeros((pairs, rope_dim, rank), BF16)
        wuk_odd[:, :rope_dim] = zero
        wuk_odd[:, rope_dim + nope :] = zero
        gain = gain_a_ref[...].astype(F32).reshape(1, d_model)
        x_norm = (unit_norm(x_ref[...].astype(F32)) * gain).astype(BF16)
        pos_row = pos_ref[...]
        pos_col = jnp.broadcast_to(pos_row.astype(F32), (rows, rows)).T
        pos_scr[...] = pos_col
        lane = lax.broadcasted_iota(jnp.int32, (rows, 2 * rope_dim), 1)
        power = lax.rem(lane, rope_dim // 2).astype(F32) * (2.0 / rope_dim)
        angle = pos_col * jnp.exp(power * -math.log(ROPE_BASE))
        cos, sin = jnp.cos(angle), jnp.sin(angle)
        first = lax.rem(lane, rope_dim) < rope_dim // 2

        def rope(v):
            ahead = pltpu.roll(v, 2 * rope_dim - rope_dim // 2, 1)
            behind = pltpu.roll(v, rope_dim // 2, 1)
            return (v * cos + jnp.where(first, -ahead, behind) * sin).astype(BF16).astype(F32)

        kv_copy.wait()
        kv = mm_nt(x_norm, wkv[...])
        c_scr[...] = unit_norm(kv[:, :rank]).astype(BF16).astype(F32)
        k_part = kv[:, rank:]
        k_new = rope(jnp.concatenate([k_part, k_part], axis=1)).T[:rope_dim]
        rope_copy.wait()

        half = seq // 2
        for j in range(half):
            both = []
            for pos in (j, j + half):
                keys = jnp.where(pos_row == pos, k_new, rope_in[pos].astype(F32))
                rope_out[pos] = keys.astype(BF16)
                both.append(keys)
            rope_keys[pl.ds(j, rows, stride=half), :] = jnp.concatenate(both, axis=0).T

        for i in range(pairs):
            if i % per_copy == 0:
                q_copy(i // per_copy).wait()
            for c in uk_copies(i):
                c.wait()
            q = mm(x_norm, wq[:, i * pair_cols : (i + 1) * pair_cols]).astype(BF16)
            qc[2 * i] = mm(q[:, :nope], wuk_even[i]).astype(BF16).astype(F32)
            qc[2 * i + 1] = mm(q[:, nope:], wuk_odd[i]).astype(BF16).astype(F32)
            both = jnp.where(lane < rope_dim, q[:, nope : 2 * nope].astype(F32), q[:, 2 * nope :].astype(F32))
            turned = rope(both)
            even, odd = jnp.where(lane < rope_dim, turned, 0.0), jnp.where(lane < rope_dim, 0.0, turned)
            q_first[2 * i] = even
            q_second[2 * i] = pltpu.roll(even, rope_dim, 1)
            q_first[2 * i + 1] = pltpu.roll(odd, rope_dim, 1)
            q_second[2 * i + 1] = odd

    for g in range(GROUPS):
        at = pl.ds(pl.multiple_of((step * GROUPS + g) * GROUP, GROUP), GROUP)
        mine = pl.ds(g * GROUP, GROUP)
        c_new = c_scr[at, :]
        lat_out[mine] = lat_ref[mine]
        row = lax.broadcasted_iota(jnp.int32, (16, rank), 0)
        for t in range(GROUP):
            pos = pos_smem[(step * GROUPS + g) * GROUP + t]
            base = pl.multiple_of((pos // 16) * 16, 16)
            old = lat_ref[g * GROUP + t, pl.ds(base, 16), :].astype(F32)
            lat_out[g * GROUP + t, pl.ds(base, 16), :] = jnp.where(row == pos - base, c_new[t : t + 1, :], old).astype(BF16)
    half = seq // 2
    key_id = lax.broadcasted_iota(jnp.int32, (GROUP, GROUP * seq), 1)
    in_half = lax.rem(key_id, GROUP * half)
    same = in_half // half == lax.broadcasted_iota(jnp.int32, (GROUP, GROUP * seq), 0)
    key_pos = (lax.rem(in_half, half) + key_id // (GROUP * half) * half).astype(F32)

    def tokens(g):
        return pl.ds(pl.multiple_of((step * GROUPS + g) * GROUP, GROUP), GROUP)

    def keys_of(g, k):
        return lat_out[pl.ds(g * GROUP, GROUP), k * half : (k + 1) * half].reshape(GROUP * half, rank)

    for g in range(GROUPS):
        first_row = pl.multiple_of((step * GROUPS + g) * GROUP * half, GROUP * half)
        turned_keys = rope_keys[pl.ds(first_row, GROUP * half), :].astype(BF16)
        q_lat = qc[:, tokens(g), :].reshape(heads * GROUP, rank).astype(BF16)
        for k, q_part in enumerate((q_first, q_second)):
            q_rope = q_part[:, tokens(g), :].reshape(heads * GROUP, 2 * rope_dim).astype(BF16)
            s_scr[g, :, k * GROUP * half : (k + 1) * GROUP * half] = mm_nt(q_lat, keys_of(g, k)) + mm_nt(q_rope, turned_keys)
    for g in range(GROUPS):
        seen = same & (key_pos <= jnp.concatenate([pos_scr[tokens(g), :]] * (GROUP * seq // rows), axis=-1))
        for h in range(0, heads, 4):
            part = pl.ds(h * GROUP, 4 * GROUP)
            scores = s_scr[g, part, :].reshape(4, GROUP, GROUP * seq) * (nope + rope_dim) ** -0.5
            scores = jnp.where(seen[None], scores, -jnp.inf)
            expd = jnp.exp(scores - jnp.max(scores, axis=-1, keepdims=True))
            prob = (expd * (1.0 / jnp.sum(expd, axis=-1, keepdims=True))).astype(BF16)
            p_scr[g, part, :] = prob.reshape(4 * GROUP, GROUP * seq)
    for g in range(GROUPS):
        out = mm(p_scr[g], jnp.concatenate([keys_of(g, 0), keys_of(g, 1)], axis=0)).astype(BF16).astype(F32)
        olat[:, tokens(g), :] = out.reshape(heads, GROUP, rank)

    @pl.when(step == pl.num_programs(0) - 1)
    def _():
        uv_copy.wait()
        v_dim = wuv.shape[-1]
        for h in range(heads):
            heads_scr[:, h * v_dim : (h + 1) * v_dim] = mm(olat[h].astype(BF16), wuv[h]).astype(BF16)
        wo_copy.wait()
        piece = 512
        for n in range(0, d_model, piece):
            part = mm(heads_scr[...], wo[:, n : n + piece])
            resid_ref[:, n : n + piece] = (x_ref[:, n : n + piece].astype(F32) + part).astype(BF16)
        gain = gain_f_ref[...].astype(F32).reshape(1, d_model)
        h_ref[...] = (unit_norm(resid_ref[...].astype(F32)) * gain).astype(BF16)


def attention(tok_in, lat_cache, rope_cache, tok_pos, attn_gain, w_query, w_kvdown, w_ukey, w_uval, w_out, ffn_gain):
    rows, d_model = tok_in.shape
    _, seq, rank = lat_cache.shape
    rope_dim = rope_cache.shape[-1]
    heads, nope, _ = w_ukey.shape
    v_dim = w_uval.shape[-1]

    def const(shape):
        return pl.BlockSpec(shape, lambda g, *_: (0,) * len(shape))

    any_spec = pl.BlockSpec(memory_space=pl.ANY)
    lat_spec = pl.BlockSpec((GROUPS * GROUP, seq, rank), lambda g, *_: (g, 0, 0))
    by_token = (seq, rope_dim, rows)
    grid_spec = pltpu.PrefetchScalarGridSpec(
        num_scalar_prefetch=1,
        grid=(rows // (GROUPS * GROUP),),
        in_specs=[const((rows, d_model)), const((1, rows)), const((d_model,)), const((d_model,)), lat_spec] + [any_spec] * 6,
        out_specs=[lat_spec, const(by_token), const((rows, d_model)), const((rows, d_model))],
        scratch_shapes=[
            pltpu.VMEM(w_query.shape, BF16),
            pltpu.VMEM(w_kvdown.shape[::-1], BF16),
            pltpu.VMEM((heads // 2, nope, rank), BF16),
            pltpu.VMEM((heads // 2, nope + 2 * rope_dim, rank), BF16),
            pltpu.VMEM(w_uval.shape, BF16),
            pltpu.VMEM(w_out.shape, BF16),
            pltpu.VMEM(by_token, BF16),
            pltpu.VMEM((rows * seq // 2, 2 * rope_dim), F32),
            pltpu.VMEM((heads, rows, rank), F32),
            pltpu.VMEM((heads, rows, 2 * rope_dim), F32),
            pltpu.VMEM((heads, rows, 2 * rope_dim), F32),
            pltpu.VMEM((heads, rows, rank), F32),
            pltpu.VMEM((rows, rank), F32),
            pltpu.VMEM((rows, rows), F32),
            pltpu.VMEM((rows, heads * v_dim), BF16),
            pltpu.VMEM((GROUPS, heads * GROUP, GROUP * seq), F32),
            pltpu.VMEM((GROUPS, heads * GROUP, GROUP * seq), BF16),
            pltpu.SemaphoreType.DMA((heads // 4 + 4 + heads,)),
        ],
    )
    lat_out, rope_out, resid, h_norm = pl.pallas_call(
        attention_kernel,
        name="attention",
        grid_spec=grid_spec,
        out_shape=[
            jax.ShapeDtypeStruct(lat_cache.shape, BF16),
            jax.ShapeDtypeStruct(by_token, BF16),
            jax.ShapeDtypeStruct((rows, d_model), BF16),
            jax.ShapeDtypeStruct((rows, d_model), BF16),
        ],
        compiler_params=pltpu.CompilerParams(vmem_limit_bytes=VMEM_LIMIT, dimension_semantics=("arbitrary",)),
    )(tok_pos, tok_in, tok_pos[None, :], attn_gain, ffn_gain, lat_cache, rope_cache.transpose(1, 2, 0),
      w_query, w_kvdown.T, w_ukey, w_uval, w_out)
    return lat_out, rope_out.transpose(2, 0, 1), resid, h_norm


def moe_kernel(
    ep, slots, h_in, resid_ref, ids_ref, wr_ref,
    shg, shu, shd, exg, exu, exd,
    out_ref,
    wbuf, h_all, w_send, w_all, pick, weigh, comb, x_all, acts, acts_sh, e_buf,
    part, part_peer, from_peer, transit, final, sh_acc,
    sl_w, y_even, y_send, slots_in, rank_home, weigh_home, comb_home, sh_first,
    w_sem, b_sem, ag_send, ag_recv, rt_send, rt_recv, rs_send, rs_recv, sl_sem, sl_send, sl_recv,
):
    rows, d_model = h_in.shape
    local, _, ff = exg.shape
    chips = ep // 2
    half = rows // 2
    pair_slots = 2 * slots
    shared_parts = shg.shape[1] // ff
    chunks = (d_model - BY_SLOT) // CHUNK
    per_slot = ff // CHUNK
    me = lax.axis_index("ep")
    chip, core = me // 2, lax.rem(me, 2)

    def device(chip_step, other_core):
        side = 1 - core if other_core else core
        return lax.rem(chip + chip_step, chips) * 2 + side

    right, left, peer = device(1, False), device(chips - 1, False), device(0, True)

    def remote(src, dst, send, recv, to):
        return pltpu.make_async_remote_copy(
            src_ref=src, dst_ref=dst, send_sem=send, recv_sem=recv,
            device_id={"ep": to}, device_id_type=pl.DeviceIdType.MESH)

    def shared_copies(i):
        cols = pl.ds(i * ff, ff)
        return [pltpu.make_async_copy(src.at[:, cols], wbuf.at[i % 2, k], w_sem.at[i % 2, k]) for k, src in enumerate((shg, shu))]

    def expert_copies(e):
        s = lax.rem(e, 2)
        return [pltpu.make_async_copy(src.at[e], wbuf.at[s, k], w_sem.at[s, k]) for k, src in enumerate((exg, exu))]

    def down_copy(c, k):
        s = lax.rem(c, 2)
        cols = pl.ds(pl.multiple_of(BY_SLOT + c * CHUNK, CHUNK), CHUNK)
        src = exd.at[k, :, cols] if k < local else shd.at[pl.ds((k - local) * ff, ff), cols]
        return pltpu.make_async_copy(src, down_tile(c, k), b_sem.at[s, k])

    def down_tile(c, k):
        return wbuf.at[lax.rem(c, 2), k // per_slot, pl.ds(0, ff), pl.ds((k % per_slot) * CHUNK, CHUNK)]

    def start_down(c):
        for k in range(local + shared_parts):
            down_copy(c, k).start()

    def slot_copy(e, s):
        return pltpu.make_async_copy(exd.at[e, :, pl.ds(0, BY_SLOT)], sl_w.at[s], sl_sem.at[s])

    def slot_copy_shared(i):
        return pltpu.make_async_copy(shd.at[pl.ds(i * ff, ff), pl.ds(0, BY_SLOT)], sl_w.at[i % 2], sl_sem.at[i % 2])

    for i in range(shared_parts):
        for c in shared_copies(i):
            c.start()
    for i in range(shared_parts):
        slot_copy_shared(i).start()

    barrier = pltpu.get_barrier_semaphore()
    others = [(dc, oc) for dc in range(chips) for oc in (False, True) if dc or oc]
    for dc, oc in others:
        pl.semaphore_signal(barrier, inc=1, device_id={"ep": device(dc, oc)}, device_id_type=pl.DeviceIdType.MESH)
    pl.semaphore_wait(barrier, len(others))

    top, low = pl.ds(0, half), pl.ds(half, half)
    top_o, low_o = pl.ds(rows, half), pl.ds(rows + half, half)
    back, far = chips - 1, chips - 2

    def gather_copy(i):
        src, dst, to = (
            (h_in, h_all.at[0, pl.ds(rows, rows)], peer),
            (h_in.at[top], h_all.at[back, top], right),
            (h_in.at[low], h_all.at[back, low], right),
            (h_in.at[low], h_all.at[1, low], left),
            (h_in.at[top], h_all.at[1, top], left),
            (h_all.at[back, top], h_all.at[far, top], right),
            (h_all.at[1, low], h_all.at[far, low], left),
            (h_all.at[back, top], h_all.at[back, top_o], peer),
            (h_all.at[1, low], h_all.at[1, low_o], peer),
            (h_all.at[back, low], h_all.at[back, low_o], peer),
            (h_all.at[1, top], h_all.at[1, top_o], peer),
            (h_all.at[far, top], h_all.at[far, top_o], peer),
            (h_all.at[far, low], h_all.at[far, low_o], peer),
        )[i]
        return remote(src, dst, ag_send.at[i], ag_recv.at[i], to)

    for i in range(5):
        gather_copy(i).start()

    logits = mm_nt(wr_ref[...], h_in[...])
    gate = jax.nn.sigmoid(logits)
    expert_id = lax.broadcasted_iota(jnp.int32, logits.shape, 0)
    listed = expert_id == ids_ref[0:1, :]
    for k in range(1, ids_ref.shape[0]):
        listed = listed | (expert_id == ids_ref[k : k + 1, :])
    total = jnp.sum(jnp.where(listed, gate, 0.0), axis=0, keepdims=True)
    w_send[...] = jnp.where(listed, ROUTE_SCALE * gate / total, -1.0)

    def mine(d):
        return pl.ds(pl.multiple_of(d * local, local), local)

    def route_copy(i):
        dc, oc = others[i]
        d = device(dc, oc)
        return remote(w_send.at[mine(d)], w_all.at[(chips - dc) % chips, int(oc)], rt_send.at[i], rt_recv.at[i], d)

    for i in range(len(others)):
        route_copy(i).start()
    w_all[0, 0] = w_send[mine(me), :]
    h_all[0, :rows] = h_in[...]

    def up(x, s, act):
        for n in range(0, ff, 512):
            cols = pl.ds(n, min(512, ff - n))
            g = mm(x[...], wbuf[s, 0, :, cols])
            u = mm(x[...], wbuf[s, 1, :, cols])
            act[:, cols] = (jax.nn.silu(g) * u).astype(BF16)

    earlier = lax.broadcasted_iota(jnp.int32, (rows, rows), 0) < lax.broadcasted_iota(jnp.int32, (rows, rows), 1)
    tri = jnp.where(earlier, 1.0, 0.0).astype(BF16)
    slot_id = lax.broadcasted_iota(jnp.int32, (pair_slots, 2 * rows), 0).astype(F32)

    def place(r):
        ranks, weights = [], []
        for q in range(2):
            w = w_all[r, q]
            has = w >= 0.0
            rank = mm(jnp.where(has, 1.0, 0.0).astype(BF16), tri)
            ranks.append(jnp.where(has, rank + q * slots, -1.0))
            weights.append(w)
        rank, w = jnp.concatenate(ranks, axis=1), jnp.concatenate(weights, axis=1)
        for e in range(local):
            at = pl.ds(e * pair_slots, pair_slots)
            hit = slot_id == rank[e : e + 1, :]
            pick[at, :] = jnp.where(hit, 1.0, 0.0).astype(BF16)
            weigh[at, :] = jnp.where(hit, w[e : e + 1, :], 0.0)
        rest = weigh[...].T
        for k in range(3):
            piece = rest.astype(BF16)
            comb[r, k] = piece
            rest = rest - piece.astype(F32)

        @pl.loop(0, d_model // 1024)
        def _(n):
            cols = pl.ds(pl.multiple_of(n * 1024, 1024), 1024)
            x = mm(pick[...], h_all[r, :, cols]).astype(BF16)
            for e in range(local):
                x_all[e, pl.ds(r * pair_slots, pair_slots), cols] = x[e * pair_slots : (e + 1) * pair_slots]

    def wait_recv(*ids):
        for i in ids:
            gather_copy(i).wait_recv()

    for c in shared_copies(0):
        c.wait()
    up(h_in, 0, acts_sh.at[0])
    for c in expert_copies(0):
        c.start()
    wait_recv(1, 3)
    for i in (5, 6, 7, 8):
        gather_copy(i).start()
    for c in shared_copies(1):
        c.wait()
    up(h_in, 1, acts_sh.at[1])
    for c in expert_copies(1):
        c.start()
    for i in range(shared_parts):
        slot_copy_shared(i).wait()
    y = None
    for i in range(shared_parts):
        y_i = mm(acts_sh[i], sl_w[i % 2])
        y = y_i if y is None else y + y_i
    sh_first[...] = y
    for e in range(2):
        slot_copy(e, e).start()

    has = w_send[...] >= 0.0
    rank_home[...] = jnp.where(has, mm(jnp.where(has, 1.0, 0.0).astype(BF16), tri), -1.0)
    home_id = lax.broadcasted_iota(jnp.int32, (slots, rows), 0).astype(F32)
    for r in range(chips):
        for q in range(2):
            at = mine(device(r, bool(q)))
            rank, w = rank_home[at, :], w_send[at, :]
            for e in range(local):
                hit = home_id == rank[e : e + 1, :]
                weigh_home[pl.ds(((r * 2 + q) * local + e) * slots, slots), :] = jnp.where(hit, w[e : e + 1, :], 0.0)
    for b in range(0, weigh_home.shape[0], 256):
        rest = weigh_home[b : b + 256, :].T
        for k in range(3):
            piece = rest.astype(BF16)
            comb_home[k, :, b : b + 256] = piece
            rest = rest - piece.astype(F32)

    for i in range(len(others)):
        route_copy(i).wait_recv()
    wait_recv(0)
    place(0)
    wait_recv(2, 4)
    for i in (9, 10):
        gather_copy(i).start()
    wait_recv(7, 9)
    place(back)
    wait_recv(8, 10)
    place(1)
    wait_recv(5, 6)
    for i in (11, 12):
        gather_copy(i).start()
    wait_recv(11, 12)
    place(far)

    def back_copy(i, p):
        dc, oc = others[i]
        return remote(y_send.at[dc, int(oc), p], slots_in.at[(chips - dc) % chips, int(oc), p], sl_send.at[i, p], sl_recv.at[i, p], device(dc, oc))

    @pl.loop(0, local // 2)
    def _(p):
        for s in range(2):
            e = 2 * p + s
            for c in expert_copies(e):
                c.wait()
            up(x_all.at[e], s, acts.at[e])

            @pl.when(p < local // 2 - 1)
            def _():
                for c in expert_copies(e + 2):
                    c.start()

            @pl.when(p == local // 2 - 1)
            def _():
                start_down(s)

            slot_copy(e, s).wait()
            y = mm(acts[e], sl_w[s])
            if s == 0:
                y_even[...] = y

            @pl.when(p < local // 2 - 1)
            def _():
                slot_copy(e + 2, s).start()

            if s == 1:
                for r in range(chips):
                    for q in range(2):
                        at = r * pair_slots + q * slots
                        both = jnp.concatenate([y_even[at : at + slots, :], y[at : at + slots]], axis=0).astype(BF16)
                        if r or q:
                            y_send[r, q, p] = both
                        else:
                            slots_in[0, 0, p] = both
                for i in range(len(others)):
                    back_copy(i, p).start()

    def rs_copy(i, c):
        src, dst, to = (
            (part_peer.at[lax.rem(c, 2)], from_peer.at[c], peer),
            (part.at[c, far, top], transit.at[0, c], right),
            (part.at[c, far, low], transit.at[1, c], left),
            (part.at[c, 1, low], final.at[0, c, low], right),
            (part.at[c, back, top], final.at[1, c, top], left),
            (part.at[c, 1, top], final.at[0, c, top], right),
            (part.at[c, back, low], final.at[1, c, low], left),
        )[i]
        return remote(src, dst, rs_send.at[i, c], rs_recv.at[i, c], to)

    def add_peer(c):
        rs_copy(0, c).wait_recv()
        for r in (far, 1, back):
            part[c, r] += from_peer[c, r]
            if r == far:
                rs_copy(1, c).start()
                rs_copy(2, c).start()
        rs_copy(3, c).start()
        rs_copy(4, c).start()
        part[c, 0] += from_peer[c, 0]

    def pass_on(c):
        rs_copy(1, c).wait_recv()
        part[c, 1, top] += transit[0, c]
        rs_copy(5, c).start()
        rs_copy(2, c).wait_recv()
        part[c, back, low] += transit[1, c]
        rs_copy(6, c).start()

    @pl.loop(0, chunks)
    def _(c):
        for k in range(local + shared_parts):
            down_copy(c, k).wait()
        for k in range(local):
            y = mm(acts[k], down_tile(c, k)[...]).astype(BF16)
            for r in range(chips):
                e_buf[r, k * pair_slots : (k + 1) * pair_slots, :] = y[r * pair_slots : (r + 1) * pair_slots]

        @pl.when(c >= 1)
        def _():
            add_peer(c - 1)

        @pl.when(c >= 2)
        def _():
            rs_copy(0, c - 2).wait_send()

        for r in range(chips):
            e_r = e_buf[r]
            z = mm(comb[r, 0], e_r) + mm(comb[r, 1], e_r) + mm(comb[r, 2], e_r)
            part[c, r] = z[:rows]
            part_peer[lax.rem(c, 2), r] = z[rows:]
        rs_copy(0, c).start()

        shared = None
        for k in range(local, local + shared_parts):
            y = mm(acts_sh[k - local], down_tile(c, k)[...])
            shared = y if shared is None else shared + y
        sh_acc[c] = shared

        @pl.when(c + 2 < chunks)
        def _():
            start_down(c + 2)

        @pl.when(c >= 2)
        def _():
            pass_on(c - 2)

    add_peer(chunks - 1)
    pass_on(chunks - 2)
    pass_on(chunks - 1)
    for p in range(local // 2):
        for i in range(len(others)):
            back_copy(i, p).wait_recv()
    back_rows = slots_in[...].reshape(ep * local * slots, BY_SLOT)
    routed = mm(comb_home[0], back_rows) + mm(comb_home[1], back_rows) + mm(comb_home[2], back_rows)
    out_ref[:, :BY_SLOT] = (resid_ref[:, :BY_SLOT].astype(F32) + sh_first[...] + routed).astype(BF16)
    for c in range(chunks):
        for i in (3, 4, 5, 6):
            rs_copy(i, c).wait_recv()
        cols = pl.ds(BY_SLOT + c * CHUNK, CHUNK)
        routed = part[c, 0] + final[0, c] + final[1, c]
        out_ref[:, cols] = (resid_ref[:, cols].astype(F32) + sh_acc[c] + routed).astype(BF16)
    for i in range(13):
        gather_copy(i).wait_send()
    for i in range(len(others)):
        route_copy(i).wait_send()

    for p in range(local // 2):
        for i in range(len(others)):
            back_copy(i, p).wait_send()
    for c in range(chunks - 2, chunks):
        rs_copy(0, c).wait_send()

    @pl.loop(0, chunks)
    def _(c):
        for i in range(1, 7):
            rs_copy(i, c).wait_send()


def moe(ep, h_norm, resid, expert_ids, w_router, sh_gate, sh_up, sh_down, ex_gate, ex_up, ex_down):
    rows, d_model = h_norm.shape
    top_k = expert_ids.shape[1]
    num_experts = w_router.shape[1]
    local, _, ff = ex_gate.shape
    chips = ep // 2
    slots = max(2, -(-2 * rows * top_k // num_experts))
    shared_parts = sh_gate.shape[1] // ff
    chunks = (d_model - BY_SLOT) // CHUNK
    pair_slots = 2 * slots
    dma = pltpu.SemaphoreType.DMA
    vmem = pl.BlockSpec(memory_space=pltpu.VMEM)
    any_spec = pl.BlockSpec(memory_space=pl.ANY)
    return pl.pallas_call(
        functools.partial(moe_kernel, ep, slots),
        name="experts",
        in_specs=[vmem] * 4 + [any_spec] * 6,
        out_specs=vmem,
        out_shape=jax.ShapeDtypeStruct((rows, d_model), BF16),
        scratch_shapes=[
            pltpu.VMEM((2, 2, d_model, ff), BF16),
            pltpu.VMEM((chips, 2 * rows, d_model), BF16),
            pltpu.VMEM((num_experts, rows), F32),
            pltpu.VMEM((chips, 2, local, rows), F32),
            pltpu.VMEM((local * pair_slots, 2 * rows), BF16),
            pltpu.VMEM((local * pair_slots, 2 * rows), F32),
            pltpu.VMEM((chips, 3, 2 * rows, local * pair_slots), BF16),
            pltpu.VMEM((local, chips * pair_slots, d_model), BF16),
            pltpu.VMEM((local, chips * pair_slots, ff), BF16),
            pltpu.VMEM((shared_parts, rows, ff), BF16),
            pltpu.VMEM((chips, local * pair_slots, CHUNK), BF16),
            pltpu.VMEM((chunks, chips, rows, CHUNK), F32),
            pltpu.VMEM((2, chips, rows, CHUNK), F32),
            pltpu.VMEM((chunks, chips, rows, CHUNK), F32),
            pltpu.VMEM((2, chunks, rows // 2, CHUNK), F32),
            pltpu.VMEM((2, chunks, rows, CHUNK), F32),
            pltpu.VMEM((chunks, rows, CHUNK), F32),
            pltpu.VMEM((2, ff, BY_SLOT), BF16),
            pltpu.VMEM((chips * pair_slots, BY_SLOT), F32),
            pltpu.VMEM((chips, 2, local // 2, pair_slots, BY_SLOT), BF16),
            pltpu.VMEM((chips, 2, local // 2, pair_slots, BY_SLOT), BF16),
            pltpu.VMEM((num_experts, rows), F32),
            pltpu.VMEM((num_experts * slots, rows), F32),
            pltpu.VMEM((3, rows, num_experts * slots), BF16),
            pltpu.VMEM((rows, BY_SLOT), F32),
            dma((2, 2)), dma((2, local + shared_parts)),
            dma((13,)), dma((13,)), dma((ep - 1,)), dma((ep - 1,)), dma((7, chunks)), dma((7, chunks)),
            dma((2,)), dma((ep - 1, local // 2)), dma((ep - 1, local // 2)),
        ],
        compiler_params=pltpu.CompilerParams(vmem_limit_bytes=VMEM_LIMIT, collective_id=0, has_side_effects=True),
    )(h_norm, resid, expert_ids.T, w_router.T, sh_gate, sh_up, sh_down, ex_gate, ex_up, ex_down)


def solution(mesh):
    ep = mesh.shape["ep"]
    row_one = P(("dp", "ep"))
    row_two = P(("dp", "ep"), None)
    row_three = P(("dp", "ep"), None, None)
    rep_one = P(None)
    rep_two = P(None, None)
    rep_three = P(None, None, None)
    exp_spec = P("ep", None, None)

    def local_step(tok_in, lat_cache, rope_cache, tok_pos, expert_ids, attn_gain, w_query, w_kvdown, w_ukey, w_uval, w_out, ffn_gain, w_router, sh_gate, sh_up, sh_down, ex_gate, ex_up, ex_down):
        lat_out, rope_out, resid, h_norm = attention(tok_in, lat_cache, rope_cache, tok_pos, attn_gain, w_query, w_kvdown, w_ukey, w_uval, w_out, ffn_gain)
        out_hidden = moe(ep, h_norm, resid, expert_ids, w_router, sh_gate, sh_up, sh_down, ex_gate, ex_up, ex_down)
        return out_hidden, lat_out, rope_out

    in_specs = (row_two, row_three, row_three, row_one, row_two, rep_one, rep_two, rep_two, rep_three, rep_three, rep_two, rep_one, rep_two, rep_two, rep_two, rep_two, exp_spec, exp_spec, exp_spec)
    out_specs = (row_two, row_three, row_three)
    return jax.shard_map(local_step, mesh=mesh, in_specs=in_specs, out_specs=out_specs, check_vma=False)
```

```python
import functools
import math

import jax
import jax.numpy as jnp
from jax import lax
from jax.experimental import pallas as pl
from jax.experimental.pallas import tpu as pltpu
from jax.sharding import PartitionSpec as P

ROUTE_SCALE = 2.827
ROPE_BASE = 10000.0
NORM_EPS = 1e-6
F32 = jnp.float32
BF16 = jnp.bfloat16
VMEM_LIMIT = 67_043_328

GROUP = 8
GROUPS = 4
CHUNK = 256
BY_SLOT = 768


def unit_norm(values):
    mean_sq = jnp.mean(jnp.square(values), axis=-1, keepdims=True)
    return values * lax.rsqrt(mean_sq + NORM_EPS)


def mm(a, b):
    return jnp.dot(a, b, preferred_element_type=F32)


def mm_nt(a, b):
    return lax.dot_general(a, b, (((1,), (1,)), ((), ())), preferred_element_type=F32)


def attention_kernel(
    pos_smem, x_ref, pos_ref, gain_a_ref, gain_f_ref,
    lat_hbm, rope_hbm, wq_hbm, wkv_hbm, wuk_hbm, wuv_hbm, wo_hbm,
    lat_out_hbm, rope_out_hbm, resid_ref, h_ref,
    wq, wkv, wuk_even, wuk_odd, wuv, wo, rope_in, rope_keys, qc, q_first, q_second, olat, c_scr, pos_scr, heads_scr, s_scr, p_scr, lat, rope_out, sem, lat_sem,
):
    step = pl.program_id(0)
    heads, nope, rank = wuk_hbm.shape
    seq, rope_dim, rows = rope_in.shape
    d_model = x_ref.shape[1]
    pairs = heads // 2
    pair_cols = 2 * (nope + rope_dim)
    per_copy = 2
    copies = pairs // per_copy
    wide = per_copy * pair_cols

    def q_copy(i):
        cols = pl.ds(i * wide, wide)
        return pltpu.make_async_copy(wq_hbm.at[:, cols], wq.at[:, cols], sem.at[i])

    kv_copy = pltpu.make_async_copy(wkv_hbm, wkv, sem.at[copies])
    uv_copy = pltpu.make_async_copy(wuv_hbm, wuv, sem.at[copies + 1])
    wo_copy = pltpu.make_async_copy(wo_hbm, wo, sem.at[copies + 2])
    rope_copy = pltpu.make_async_copy(rope_hbm, rope_in, sem.at[copies + 3])
    rope_back = pltpu.make_async_copy(rope_out, rope_out_hbm, sem.at[copies + 4 + heads])
    block = GROUPS * GROUP
    blocks = rows // block

    def lat_copy(b):
        at = pl.ds(b * block, block)
        return pltpu.make_async_copy(lat_hbm.at[at], lat.at[at], lat_sem.at[0, b])

    def lat_back(b):
        at = pl.ds(b * block, block)
        return pltpu.make_async_copy(lat.at[at], lat_out_hbm.at[at], lat_sem.at[1, b])


    def uk_copies(i):
        even = pltpu.make_async_copy(wuk_hbm.at[2 * i], wuk_even.at[i], sem.at[copies + 4 + 2 * i])
        odd = pltpu.make_async_copy(wuk_hbm.at[2 * i + 1], wuk_odd.at[i, rope_dim : rope_dim + nope], sem.at[copies + 5 + 2 * i])
        return even, odd

    @pl.when(step == 0)
    def _():
        kv_copy.start()
        rope_copy.start()
        for i in range(copies):
            q_copy(i).start()
            for j in range(per_copy):
                for c in uk_copies(i * per_copy + j):
                    c.start()
        for b in range(blocks):
            lat_copy(b).start()
        uv_copy.start()
        wo_copy.start()
        zero = jnp.zeros((pairs, rope_dim, rank), BF16)
        wuk_odd[:, :rope_dim] = zero
        wuk_odd[:, rope_dim + nope :] = zero
        gain = gain_a_ref[...].astype(F32).reshape(1, d_model)
        x_norm = (unit_norm(x_ref[...].astype(F32)) * gain).astype(BF16)
        pos_row = pos_ref[...]
        pos_col = jnp.broadcast_to(pos_row.astype(F32), (rows, rows)).T
        pos_scr[...] = pos_col
        lane = lax.broadcasted_iota(jnp.int32, (rows, 2 * rope_dim), 1)
        power = lax.rem(lane, rope_dim // 2).astype(F32) * (2.0 / rope_dim)
        angle = pos_col * jnp.exp(power * -math.log(ROPE_BASE))
        cos, sin = jnp.cos(angle), jnp.sin(angle)
        first = lax.rem(lane, rope_dim) < rope_dim // 2

        def rope(v):
            ahead = pltpu.roll(v, 2 * rope_dim - rope_dim // 2, 1)
            behind = pltpu.roll(v, rope_dim // 2, 1)
            return (v * cos + jnp.where(first, -ahead, behind) * sin).astype(BF16).astype(F32)

        kv_copy.wait()
        kv = mm_nt(x_norm, wkv[...])
        c_scr[...] = unit_norm(kv[:, :rank]).astype(BF16).astype(F32)
        k_part = kv[:, rank:]
        k_new = rope(jnp.concatenate([k_part, k_part], axis=1)).T[:rope_dim]
        rope_copy.wait()

        half = seq // 2

        def turn_keys(j):
            both = []
            for pos in (j, j + half):
                keys = jnp.where(pos_row == pos, k_new, rope_in[pos].astype(F32))
                rope_out[pos] = keys.astype(BF16)
                both.append(keys)
            rope_keys[pl.ds(j, rows, stride=half), :] = jnp.concatenate(both, axis=0).T

        for i in range(pairs):
            if i % per_copy == 0:
                q_copy(i // per_copy).wait()
                for k in range(per_copy):
                    for c in uk_copies(i + k):
                        c.wait()
                q_wide = mm(x_norm, wq[:, i * pair_cols : i * pair_cols + wide]).astype(BF16)
            q = q_wide[:, i % per_copy * pair_cols : (i % per_copy + 1) * pair_cols]
            qc[2 * i] = mm(q[:, :nope], wuk_even[i]).astype(BF16).astype(F32)
            qc[2 * i + 1] = mm(q[:, nope:], wuk_odd[i]).astype(BF16).astype(F32)
            both = jnp.where(lane < rope_dim, q[:, nope : 2 * nope].astype(F32), q[:, 2 * nope :].astype(F32))
            turned = rope(both)
            even, odd = jnp.where(lane < rope_dim, turned, 0.0), jnp.where(lane < rope_dim, 0.0, turned)
            q_first[2 * i] = even
            q_second[2 * i] = pltpu.roll(even, rope_dim, 1)
            q_first[2 * i + 1] = pltpu.roll(odd, rope_dim, 1)
            q_second[2 * i + 1] = odd
            for j in range(i * half // pairs, (i + 1) * half // pairs):
                turn_keys(j)
        rope_back.start()

    lat_copy(step).wait()
    row = lax.broadcasted_iota(jnp.int32, (16, rank), 0)
    for g in range(GROUPS):
        c_new = c_scr[pl.ds(pl.multiple_of((step * GROUPS + g) * GROUP, GROUP), GROUP), :]
        for t in range(GROUP):
            token = (step * GROUPS + g) * GROUP + t
            pos = pos_smem[token]
            base = pl.multiple_of((pos // 16) * 16, 16)
            old = lat[token, pl.ds(base, 16), :].astype(F32)
            lat[token, pl.ds(base, 16), :] = jnp.where(row == pos - base, c_new[t : t + 1, :], old).astype(BF16)
    half = seq // 2
    key_id = lax.broadcasted_iota(jnp.int32, (GROUP, GROUP * seq), 1)
    in_half = lax.rem(key_id, GROUP * half)
    same = in_half // half == lax.broadcasted_iota(jnp.int32, (GROUP, GROUP * seq), 0)
    key_pos = (lax.rem(in_half, half) + key_id // (GROUP * half) * half).astype(F32)

    def tokens(g):
        return pl.ds(pl.multiple_of((step * GROUPS + g) * GROUP, GROUP), GROUP)

    def keys_of(g, k):
        return lat[tokens(g), k * half : (k + 1) * half].reshape(GROUP * half, rank)

    for g in range(GROUPS):
        first_row = pl.multiple_of((step * GROUPS + g) * GROUP * half, GROUP * half)
        turned_keys = rope_keys[pl.ds(first_row, GROUP * half), :].astype(BF16)
        q_lat = qc[:, tokens(g), :].reshape(heads * GROUP, rank).astype(BF16)
        for k, q_part in enumerate((q_first, q_second)):
            q_rope = q_part[:, tokens(g), :].reshape(heads * GROUP, 2 * rope_dim).astype(BF16)
            s_scr[g, :, k * GROUP * half : (k + 1) * GROUP * half] = mm_nt(q_lat, keys_of(g, k)) + mm_nt(q_rope, turned_keys)
    lat_back(step).start()
    for g in range(GROUPS):
        seen = same & (key_pos <= jnp.concatenate([pos_scr[tokens(g), :]] * (GROUP * seq // rows), axis=-1))
        for h in range(0, heads, 4):
            part = pl.ds(h * GROUP, 4 * GROUP)
            scores = s_scr[g, part, :].reshape(4, GROUP, GROUP * seq) * (nope + rope_dim) ** -0.5
            scores = jnp.where(seen[None], scores, -jnp.inf)
            expd = jnp.exp(scores - jnp.max(scores, axis=-1, keepdims=True))
            prob = (expd * (1.0 / jnp.sum(expd, axis=-1, keepdims=True))).astype(BF16)
            p_scr[g, part, :] = prob.reshape(4 * GROUP, GROUP * seq)
    for g in range(GROUPS):
        out = mm(p_scr[g], jnp.concatenate([keys_of(g, 0), keys_of(g, 1)], axis=0)).astype(BF16).astype(F32)
        olat[:, tokens(g), :] = out.reshape(heads, GROUP, rank)

    @pl.when(step == pl.num_programs(0) - 1)
    def _():
        uv_copy.wait()
        v_dim = wuv.shape[-1]
        for h in range(heads):
            heads_scr[:, h * v_dim : (h + 1) * v_dim] = mm(olat[h].astype(BF16), wuv[h]).astype(BF16)
        wo_copy.wait()
        piece = 512
        for n in range(0, d_model, piece):
            part = mm(heads_scr[...], wo[:, n : n + piece])
            resid_ref[:, n : n + piece] = (x_ref[:, n : n + piece].astype(F32) + part).astype(BF16)
        gain = gain_f_ref[...].astype(F32).reshape(1, d_model)
        h_ref[...] = (unit_norm(resid_ref[...].astype(F32)) * gain).astype(BF16)
        for b in range(blocks):
            lat_back(b).wait()
        rope_back.wait()


def attention(tok_in, lat_cache, rope_cache, tok_pos, attn_gain, w_query, w_kvdown, w_ukey, w_uval, w_out, ffn_gain):
    rows, d_model = tok_in.shape
    _, seq, rank = lat_cache.shape
    rope_dim = rope_cache.shape[-1]
    heads, nope, _ = w_ukey.shape
    v_dim = w_uval.shape[-1]

    def const(shape):
        return pl.BlockSpec(shape, lambda g, *_: (0,) * len(shape))

    any_spec = pl.BlockSpec(memory_space=pl.ANY)
    by_token = (seq, rope_dim, rows)
    grid_spec = pltpu.PrefetchScalarGridSpec(
        num_scalar_prefetch=1,
        grid=(rows // (GROUPS * GROUP),),
        in_specs=[const((rows, d_model)), const((1, rows)), const((d_model,)), const((d_model,))] + [any_spec] * 7,
        out_specs=[any_spec, any_spec, const((rows, d_model)), const((rows, d_model))],
        scratch_shapes=[
            pltpu.VMEM(w_query.shape, BF16),
            pltpu.VMEM(w_kvdown.shape[::-1], BF16),
            pltpu.VMEM((heads // 2, nope, rank), BF16),
            pltpu.VMEM((heads // 2, nope + 2 * rope_dim, rank), BF16),
            pltpu.VMEM(w_uval.shape, BF16),
            pltpu.VMEM(w_out.shape, BF16),
            pltpu.VMEM(by_token, BF16),
            pltpu.VMEM((rows * seq // 2, 2 * rope_dim), F32),
            pltpu.VMEM((heads, rows, rank), F32),
            pltpu.VMEM((heads, rows, 2 * rope_dim), F32),
            pltpu.VMEM((heads, rows, 2 * rope_dim), F32),
            pltpu.VMEM((heads, rows, rank), F32),
            pltpu.VMEM((rows, rank), F32),
            pltpu.VMEM((rows, rows), F32),
            pltpu.VMEM((rows, heads * v_dim), BF16),
            pltpu.VMEM((GROUPS, heads * GROUP, GROUP * seq), F32),
            pltpu.VMEM((GROUPS, heads * GROUP, GROUP * seq), BF16),
            pltpu.VMEM(lat_cache.shape, BF16),
            pltpu.VMEM(by_token, BF16),
            pltpu.SemaphoreType.DMA((heads // 4 + 5 + heads,)),
            pltpu.SemaphoreType.DMA((2, rows // (GROUPS * GROUP))),
        ],
    )
    lat_out, rope_out, resid, h_norm = pl.pallas_call(
        attention_kernel,
        name="attention",
        grid_spec=grid_spec,
        out_shape=[
            jax.ShapeDtypeStruct(lat_cache.shape, BF16),
            jax.ShapeDtypeStruct(by_token, BF16),
            jax.ShapeDtypeStruct((rows, d_model), BF16),
            jax.ShapeDtypeStruct((rows, d_model), BF16),
        ],
        compiler_params=pltpu.CompilerParams(vmem_limit_bytes=VMEM_LIMIT, dimension_semantics=("arbitrary",)),
    )(tok_pos, tok_in, tok_pos[None, :], attn_gain, ffn_gain, lat_cache, rope_cache.transpose(1, 2, 0),
      w_query, w_kvdown.T, w_ukey, w_uval, w_out)
    return lat_out, rope_out.transpose(2, 0, 1), resid, h_norm


def moe_kernel(
    ep, slots, h_in, resid_ref, ids_ref, wr_ref,
    shg, shu, shd, exg, exu, exd,
    out_ref,
    wbuf, h_all, w_send, w_all, pick, weigh, comb, x_all, acts, acts_sh, e_buf,
    part, part_peer, from_peer, transit, final, sh_acc,
    sl_w, y_even, y_send, slots_in, rank_home, weigh_home, comb_home, sh_first,
    w_sem, b_sem, ag_send, ag_recv, rt_send, rt_recv, rs_send, rs_recv, sl_sem, sl_send, sl_recv,
):
    rows, d_model = h_in.shape
    local, _, ff = exg.shape
    chips = ep // 2
    half = rows // 2
    pair_slots = 2 * slots
    shared_parts = shg.shape[1] // ff
    chunks = (d_model - BY_SLOT) // CHUNK
    per_slot = ff // CHUNK
    me = lax.axis_index("ep")
    chip, core = me // 2, lax.rem(me, 2)

    def device(chip_step, other_core):
        side = 1 - core if other_core else core
        return lax.rem(chip + chip_step, chips) * 2 + side

    right, left, peer = device(1, False), device(chips - 1, False), device(0, True)

    def remote(src, dst, send, recv, to):
        return pltpu.make_async_remote_copy(
            src_ref=src, dst_ref=dst, send_sem=send, recv_sem=recv,
            device_id={"ep": to}, device_id_type=pl.DeviceIdType.MESH)

    def shared_copies(i):
        cols = pl.ds(i * ff, ff)
        return [pltpu.make_async_copy(src.at[:, cols], wbuf.at[i % 2, k], w_sem.at[i % 2, k]) for k, src in enumerate((shg, shu))]

    def expert_copies(e):
        s = lax.rem(e, 2)
        return [pltpu.make_async_copy(src.at[e], wbuf.at[s, k], w_sem.at[s, k]) for k, src in enumerate((exg, exu))]

    def down_copy(c, k):
        s = lax.rem(c, 2)
        cols = pl.ds(pl.multiple_of(BY_SLOT + c * CHUNK, CHUNK), CHUNK)
        src = exd.at[k, :, cols] if k < local else shd.at[pl.ds((k - local) * ff, ff), cols]
        return pltpu.make_async_copy(src, down_tile(c, k), b_sem.at[s, k])

    def down_tile(c, k):
        return wbuf.at[lax.rem(c, 2), k // per_slot, pl.ds(0, ff), pl.ds((k % per_slot) * CHUNK, CHUNK)]

    def start_down(c):
        for k in range(local + shared_parts):
            down_copy(c, k).start()

    def slot_copy(e, s):
        return pltpu.make_async_copy(exd.at[e, :, pl.ds(0, BY_SLOT)], sl_w.at[s], sl_sem.at[s])

    def slot_copy_shared(i):
        return pltpu.make_async_copy(shd.at[pl.ds(i * ff, ff), pl.ds(0, BY_SLOT)], sl_w.at[i % 2], sl_sem.at[i % 2])

    for i in range(shared_parts):
        for c in shared_copies(i):
            c.start()
    for i in range(shared_parts):
        slot_copy_shared(i).start()

    barrier = pltpu.get_barrier_semaphore()
    others = [(dc, oc) for dc in (chips - 2, 1, chips - 1, 0) for oc in (False, True) if dc or oc]
    for dc, oc in others:
        pl.semaphore_signal(barrier, inc=1, device_id={"ep": device(dc, oc)}, device_id_type=pl.DeviceIdType.MESH)
    pl.semaphore_wait(barrier, len(others))

    top, low = pl.ds(0, half), pl.ds(half, half)
    top_o, low_o = pl.ds(rows, half), pl.ds(rows + half, half)
    back, far = chips - 1, chips - 2

    def gather_copy(i):
        src, dst, to = (
            (h_in, h_all.at[0, pl.ds(rows, rows)], peer),
            (h_in.at[top], h_all.at[back, top], right),
            (h_in.at[low], h_all.at[back, low], right),
            (h_in.at[low], h_all.at[1, low], left),
            (h_in.at[top], h_all.at[1, top], left),
            (h_all.at[back, top], h_all.at[far, top], right),
            (h_all.at[1, low], h_all.at[far, low], left),
            (h_all.at[back, top], h_all.at[back, top_o], peer),
            (h_all.at[1, low], h_all.at[1, low_o], peer),
            (h_all.at[back, low], h_all.at[back, low_o], peer),
            (h_all.at[1, top], h_all.at[1, top_o], peer),
            (h_all.at[far, top], h_all.at[far, top_o], peer),
            (h_all.at[far, low], h_all.at[far, low_o], peer),
        )[i]
        return remote(src, dst, ag_send.at[i], ag_recv.at[i], to)

    for i in range(5):
        gather_copy(i).start()

    logits = mm_nt(wr_ref[...], h_in[...])
    gate = jax.nn.sigmoid(logits)
    expert_id = lax.broadcasted_iota(jnp.int32, logits.shape, 0)
    listed = expert_id == ids_ref[0:1, :]
    for k in range(1, ids_ref.shape[0]):
        listed = listed | (expert_id == ids_ref[k : k + 1, :])
    total = jnp.sum(jnp.where(listed, gate, 0.0), axis=0, keepdims=True)
    w_send[...] = jnp.where(listed, ROUTE_SCALE * gate / total, -1.0)

    def mine(d):
        return pl.ds(pl.multiple_of(d * local, local), local)

    def route_copy(i):
        dc, oc = others[i]
        d = device(dc, oc)
        return remote(w_send.at[mine(d)], w_all.at[(chips - dc) % chips, int(oc)], rt_send.at[i], rt_recv.at[i], d)

    for i in range(len(others)):
        route_copy(i).start()
    w_all[0, 0] = w_send[mine(me), :]
    h_all[0, :rows] = h_in[...]

    def up(x, s, act):
        for n in range(0, ff, 512):
            cols = pl.ds(n, min(512, ff - n))
            g = mm(x[...], wbuf[s, 0, :, cols])
            u = mm(x[...], wbuf[s, 1, :, cols])
            act[:, cols] = (jax.nn.silu(g) * u).astype(BF16)

    earlier = lax.broadcasted_iota(jnp.int32, (rows, rows), 0) < lax.broadcasted_iota(jnp.int32, (rows, rows), 1)
    tri = jnp.where(earlier, 1.0, 0.0).astype(BF16)
    slot_id = lax.broadcasted_iota(jnp.int32, (pair_slots, 2 * rows), 0).astype(F32)

    def place(r):
        ranks, weights = [], []
        for q in range(2):
            w = w_all[r, q]
            has = w >= 0.0
            rank = mm(jnp.where(has, 1.0, 0.0).astype(BF16), tri)
            ranks.append(jnp.where(has, rank + q * slots, -1.0))
            weights.append(w)
        rank, w = jnp.concatenate(ranks, axis=1), jnp.concatenate(weights, axis=1)
        for e in range(local):
            at = pl.ds(e * pair_slots, pair_slots)
            hit = slot_id == rank[e : e + 1, :]
            pick[at, :] = jnp.where(hit, 1.0, 0.0).astype(BF16)
            weigh[at, :] = jnp.where(hit, w[e : e + 1, :], 0.0)
        rest = weigh[...].T
        for k in range(3):
            piece = rest.astype(BF16)
            comb[r, k] = piece
            rest = rest - piece.astype(F32)

        @pl.loop(0, d_model // 1024)
        def _(n):
            cols = pl.ds(pl.multiple_of(n * 1024, 1024), 1024)
            x = mm(pick[...], h_all[r, :, cols]).astype(BF16)
            for e in range(local):
                x_all[e, pl.ds(r * pair_slots, pair_slots), cols] = x[e * pair_slots : (e + 1) * pair_slots]

    def wait_recv(*ids):
        for i in ids:
            gather_copy(i).wait_recv()

    for c in shared_copies(0):
        c.wait()
    up(h_in, 0, acts_sh.at[0])
    for c in expert_copies(0):
        c.start()
    wait_recv(1, 3)
    for i in (5, 6, 7, 8):
        gather_copy(i).start()
    for c in shared_copies(1):
        c.wait()
    up(h_in, 1, acts_sh.at[1])
    for c in expert_copies(1):
        c.start()
    for i in range(shared_parts):
        slot_copy_shared(i).wait()
    y = None
    for i in range(shared_parts):
        y_i = mm(acts_sh[i], sl_w[i % 2])
        y = y_i if y is None else y + y_i
    sh_first[...] = y
    for e in range(2):
        slot_copy(e, e).start()

    has = w_send[...] >= 0.0
    rank_home[...] = jnp.where(has, mm(jnp.where(has, 1.0, 0.0).astype(BF16), tri), -1.0)
    home_id = lax.broadcasted_iota(jnp.int32, (slots, rows), 0).astype(F32)
    for r in range(chips):
        for q in range(2):
            at = mine(device(r, bool(q)))
            rank, w = rank_home[at, :], w_send[at, :]
            for e in range(local):
                hit = home_id == rank[e : e + 1, :]
                weigh_home[pl.ds(((r * 2 + q) * local + e) * slots, slots), :] = jnp.where(hit, w[e : e + 1, :], 0.0)
    for b in range(0, weigh_home.shape[0], 256):
        rest = weigh_home[b : b + 256, :].T
        for k in range(3):
            piece = rest.astype(BF16)
            comb_home[k, :, b : b + 256] = piece
            rest = rest - piece.astype(F32)

    for i in range(len(others)):
        route_copy(i).wait_recv()
    wait_recv(0)
    place(0)
    wait_recv(2, 4)
    for i in (9, 10):
        gather_copy(i).start()
    wait_recv(7, 9)
    place(back)
    wait_recv(8, 10)
    place(1)
    wait_recv(5, 6)
    for i in (11, 12):
        gather_copy(i).start()
    wait_recv(11, 12)
    place(far)

    def back_copy(i, p):
        dc, oc = others[i]
        return remote(y_send.at[dc, int(oc), p], slots_in.at[(chips - dc) % chips, int(oc), p], sl_send.at[i, p], sl_recv.at[i, p], device(dc, oc))

    @pl.loop(0, local // 2)
    def _(p):
        for s in range(2):
            e = 2 * p + s
            for c in expert_copies(e):
                c.wait()
            up(x_all.at[e], s, acts.at[e])

            @pl.when(p < local // 2 - 1)
            def _():
                for c in expert_copies(e + 2):
                    c.start()

            @pl.when(p == local // 2 - 1)
            def _():
                start_down(s)

            slot_copy(e, s).wait()
            y = mm(acts[e], sl_w[s])
            if s == 0:
                y_even[...] = y

            @pl.when(p < local // 2 - 1)
            def _():
                slot_copy(e + 2, s).start()

            if s == 1:
                for r in range(chips):
                    for q in range(2):
                        at = r * pair_slots + q * slots
                        both = jnp.concatenate([y_even[at : at + slots, :], y[at : at + slots]], axis=0).astype(BF16)
                        if r or q:
                            y_send[r, q, p] = both
                        else:
                            slots_in[0, 0, p] = both
                for i in range(len(others)):
                    back_copy(i, p).start()

    def rs_copy(i, c):
        src, dst, to = (
            (part_peer.at[lax.rem(c, 2)], from_peer.at[c], peer),
            (part.at[c, far, top], transit.at[0, c], right),
            (part.at[c, far, low], transit.at[1, c], left),
            (part.at[c, 1, low], final.at[0, c, low], right),
            (part.at[c, back, top], final.at[1, c, top], left),
            (part.at[c, 1, top], final.at[0, c, top], right),
            (part.at[c, back, low], final.at[1, c, low], left),
        )[i]
        return remote(src, dst, rs_send.at[i, c], rs_recv.at[i, c], to)

    def add_peer(c):
        rs_copy(0, c).wait_recv()
        for r in (far, 1, back):
            part[c, r] += from_peer[c, r]
            if r == far:
                rs_copy(1, c).start()
                rs_copy(2, c).start()
        rs_copy(3, c).start()
        rs_copy(4, c).start()
        part[c, 0] += from_peer[c, 0]

    def pass_on(c):
        rs_copy(1, c).wait_recv()
        part[c, 1, top] += transit[0, c]
        rs_copy(5, c).start()
        rs_copy(2, c).wait_recv()
        part[c, back, low] += transit[1, c]
        rs_copy(6, c).start()

    @pl.loop(0, chunks)
    def _(c):
        for k in range(local + shared_parts):
            down_copy(c, k).wait()
        for k in range(local):
            y = mm(acts[k], down_tile(c, k)[...]).astype(BF16)
            for r in range(chips):
                e_buf[r, k * pair_slots : (k + 1) * pair_slots, :] = y[r * pair_slots : (r + 1) * pair_slots]

        @pl.when(c >= 1)
        def _():
            add_peer(c - 1)

        @pl.when(c >= 2)
        def _():
            rs_copy(0, c - 2).wait_send()

        for r in range(chips):
            e_r = e_buf[r]
            z = mm(comb[r, 0], e_r) + mm(comb[r, 1], e_r) + mm(comb[r, 2], e_r)
            part[c, r] = z[:rows]
            part_peer[lax.rem(c, 2), r] = z[rows:]
        rs_copy(0, c).start()

        shared = None
        for k in range(local, local + shared_parts):
            y = mm(acts_sh[k - local], down_tile(c, k)[...])
            shared = y if shared is None else shared + y
        sh_acc[c] = shared

        @pl.when(c + 2 < chunks)
        def _():
            start_down(c + 2)

        @pl.when(c >= 2)
        def _():
            pass_on(c - 2)

    add_peer(chunks - 1)
    pass_on(chunks - 2)
    pass_on(chunks - 1)
    for p in range(local // 2):
        for i in range(len(others)):
            back_copy(i, p).wait_recv()
    back_rows = slots_in[...].reshape(ep * local * slots, BY_SLOT)
    routed = mm(comb_home[0], back_rows) + mm(comb_home[1], back_rows) + mm(comb_home[2], back_rows)
    out_ref[:, :BY_SLOT] = (resid_ref[:, :BY_SLOT].astype(F32) + sh_first[...] + routed).astype(BF16)
    for c in range(chunks):
        for i in (3, 4, 5, 6):
            rs_copy(i, c).wait_recv()
        cols = pl.ds(BY_SLOT + c * CHUNK, CHUNK)
        routed = part[c, 0] + final[0, c] + final[1, c]
        out_ref[:, cols] = (resid_ref[:, cols].astype(F32) + sh_acc[c] + routed).astype(BF16)
    for i in range(13):
        gather_copy(i).wait_send()
    for i in range(len(others)):
        route_copy(i).wait_send()

    for p in range(local // 2):
        for i in range(len(others)):
            back_copy(i, p).wait_send()
    for c in range(chunks - 2, chunks):
        rs_copy(0, c).wait_send()

    @pl.loop(0, chunks)
    def _(c):
        for i in range(1, 7):
            rs_copy(i, c).wait_send()


def moe(ep, h_norm, resid, expert_ids, w_router, sh_gate, sh_up, sh_down, ex_gate, ex_up, ex_down):
    rows, d_model = h_norm.shape
    top_k = expert_ids.shape[1]
    num_experts = w_router.shape[1]
    local, _, ff = ex_gate.shape
    chips = ep // 2
    slots = max(2, -(-2 * rows * top_k // num_experts))
    shared_parts = sh_gate.shape[1] // ff
    chunks = (d_model - BY_SLOT) // CHUNK
    pair_slots = 2 * slots
    dma = pltpu.SemaphoreType.DMA
    vmem = pl.BlockSpec(memory_space=pltpu.VMEM)
    any_spec = pl.BlockSpec(memory_space=pl.ANY)
    return pl.pallas_call(
        functools.partial(moe_kernel, ep, slots),
        name="experts",
        in_specs=[vmem] * 4 + [any_spec] * 6,
        out_specs=vmem,
        out_shape=jax.ShapeDtypeStruct((rows, d_model), BF16),
        scratch_shapes=[
            pltpu.VMEM((2, 2, d_model, ff), BF16),
            pltpu.VMEM((chips, 2 * rows, d_model), BF16),
            pltpu.VMEM((num_experts, rows), F32),
            pltpu.VMEM((chips, 2, local, rows), F32),
            pltpu.VMEM((local * pair_slots, 2 * rows), BF16),
            pltpu.VMEM((local * pair_slots, 2 * rows), F32),
            pltpu.VMEM((chips, 3, 2 * rows, local * pair_slots), BF16),
            pltpu.VMEM((local, chips * pair_slots, d_model), BF16),
            pltpu.VMEM((local, chips * pair_slots, ff), BF16),
            pltpu.VMEM((shared_parts, rows, ff), BF16),
            pltpu.VMEM((chips, local * pair_slots, CHUNK), BF16),
            pltpu.VMEM((chunks, chips, rows, CHUNK), F32),
            pltpu.VMEM((2, chips, rows, CHUNK), F32),
            pltpu.VMEM((chunks, chips, rows, CHUNK), F32),
            pltpu.VMEM((2, chunks, rows // 2, CHUNK), F32),
            pltpu.VMEM((2, chunks, rows, CHUNK), F32),
            pltpu.VMEM((chunks, rows, CHUNK), F32),
            pltpu.VMEM((2, ff, BY_SLOT), BF16),
            pltpu.VMEM((chips * pair_slots, BY_SLOT), F32),
            pltpu.VMEM((chips, 2, local // 2, pair_slots, BY_SLOT), BF16),
            pltpu.VMEM((chips, 2, local // 2, pair_slots, BY_SLOT), BF16),
            pltpu.VMEM((num_experts, rows), F32),
            pltpu.VMEM((num_experts * slots, rows), F32),
            pltpu.VMEM((3, rows, num_experts * slots), BF16),
            pltpu.VMEM((rows, BY_SLOT), F32),
            dma((2, 2)), dma((2, local + shared_parts)),
            dma((13,)), dma((13,)), dma((ep - 1,)), dma((ep - 1,)), dma((7, chunks)), dma((7, chunks)),
            dma((2,)), dma((ep - 1, local // 2)), dma((ep - 1, local // 2)),
        ],
        compiler_params=pltpu.CompilerParams(vmem_limit_bytes=VMEM_LIMIT, collective_id=0, has_side_effects=True),
    )(h_norm, resid, expert_ids.T, w_router.T, sh_gate, sh_up, sh_down, ex_gate, ex_up, ex_down)


def solution(mesh):
    ep = mesh.shape["ep"]
    row_one = P(("dp", "ep"))
    row_two = P(("dp", "ep"), None)
    row_three = P(("dp", "ep"), None, None)
    rep_one = P(None)
    rep_two = P(None, None)
    rep_three = P(None, None, None)
    exp_spec = P("ep", None, None)

    def local_step(tok_in, lat_cache, rope_cache, tok_pos, expert_ids, attn_gain, w_query, w_kvdown, w_ukey, w_uval, w_out, ffn_gain, w_router, sh_gate, sh_up, sh_down, ex_gate, ex_up, ex_down):
        lat_out, rope_out, resid, h_norm = attention(tok_in, lat_cache, rope_cache, tok_pos, attn_gain, w_query, w_kvdown, w_ukey, w_uval, w_out, ffn_gain)
        out_hidden = moe(ep, h_norm, resid, expert_ids, w_router, sh_gate, sh_up, sh_down, ex_gate, ex_up, ex_down)
        return out_hidden, lat_out, rope_out

    in_specs = (row_two, row_three, row_three, row_one, row_two, rep_one, rep_two, rep_two, rep_three, rep_three, rep_two, rep_one, rep_two, rep_two, rep_two, rep_two, exp_spec, exp_spec, exp_spec)
    out_specs = (row_two, row_three, row_three)
    return jax.shard_map(local_step, mesh=mesh, in_specs=in_specs, out_specs=out_specs, check_vma=False)
```
